128 devices in a mesh: gx: 4 (over y_hi, core), gy: 8 (over y_lo, z), gz: 4 (over x).
Axes of the slice: x: 4, y: 4 (y_hi: 2, y_lo: 2; y = y_hi * 2 + y_lo), z: 4, core: 2. Of those that a mesh axis runs over, the one named last changes fastest.
Arguments:
- start_field: float32 [256, 512, 1024], P('gx', 'gy', 'gz'), may hold values from -6 to 6
- right_side: float32 [256, 512, 1024], P('gx', 'gy', 'gz'), may hold values from -6 to 6
Outputs:
- corrected: float32 [256, 512, 1024], P('gx', 'gy', 'gz')
The draws below stay inside these ranges and needn't reach their ends.
All inputs are finite; a program needn't handle non-finite values.
Results may differ from the reference program's by a relative error of at most 0.00002.
Values sent between devices are 32-bit elements; how exact they have to be, the bound alone decides.
A program may use at most 128 MiB of HBM per device.

```python
import jax
import jax.numpy as jnp
from jax import lax

FINE_SWEEPS = 2
COARSE_SWEEPS = 4
NX = 256
NY = 512
NZ = 1024


def draw_right_side(key, part):
    noise_field = jnp.clip(jax.random.normal(key, (NX, NY, NZ), jnp.float32), -6.0, 6.0)
    return noise_field


def levels(stream_key, dims, shards, smallest, top_value):
    def one(position, shards_of):
        draws = jax.random.uniform(jax.random.fold_in(jax.random.fold_in(stream_key, 6), position), (shards_of,), jnp.float32, smallest / len(shards), top_value / len(shards))
        return jnp.repeat(jnp.exp(draws), dims[position] // shards_of).reshape((-1,) + (1,) * (len(dims) - position - 1))

    factor_of = one(*shards[0])
    for cut in shards[1:]:
        factor_of = factor_of * one(*cut)
    return factor_of


def bell_draw(key, shape, spread, reach, pieces=(), kind=jnp.bfloat16):
    drawn = jax.random.normal(key, shape, jnp.float32) * spread
    if len(pieces) > 0:
        drawn = levels(key, shape, pieces, -0.22, 0.18) * drawn
    return jnp.clip(drawn, min=-reach, max=reach).astype(kind)


def setup_inputs(seed: int = 0) -> dict:
    seeds = jax.random.split(jax.random.key(seed), 3)
    start_field = bell_draw(seeds[0], (NX, NY, NZ), 1.0, 6.0, ((0, 4), (1, 8), (2, 4)), jnp.float32)
    right_side = draw_right_side(jax.random.fold_in(seeds[2], 71), 0)
    return {"start_field": start_field, "right_side": right_side}


relaxation = 6.0 / 7.0


def apply_stencil(values):
    padded = jnp.pad(values, 1)
    beside = padded[2:, 1:-1, 1:-1] + padded[:-2, 1:-1, 1:-1]
    beside = beside + padded[1:-1, 2:, 1:-1] + padded[1:-1, :-2, 1:-1]
    beside = beside + padded[1:-1, 1:-1, 2:] + padded[1:-1, 1:-1, :-2]
    return 6.0 * values - beside


def restrict_axis(values, which_axis):
    length = values.shape[which_axis]
    half_len = length // 2
    even_rows = lax.slice_in_dim(values, 0, length, 2, which_axis)
    odd_rows = lax.slice_in_dim(values, 1, length, 2, which_axis)
    zero_row = jnp.zeros_like(lax.slice_in_dim(even_rows, 0, 1, 1, which_axis))
    following = jnp.concatenate([lax.slice_in_dim(even_rows, 1, half_len, 1, which_axis), zero_row], which_axis)
    return 0.25 * even_rows + 0.5 * odd_rows + 0.25 * following


def prolong_axis(values, which_axis):
    length = values.shape[which_axis]
    zero_row = jnp.zeros_like(lax.slice_in_dim(values, 0, 1, 1, which_axis))
    previous = jnp.concatenate([zero_row, lax.slice_in_dim(values, 0, length - 1, 1, which_axis)], which_axis)
    even_rows = 0.5 * (previous + values)
    paired = jnp.stack([even_rows, values], which_axis + 1)
    new_shape = list(values.shape)
    new_shape[which_axis] = 2 * length
    return jnp.reshape(paired, new_shape)


def reference(start_field, right_side):
    smoothed = start_field
    for sweep_num in range(FINE_SWEEPS):
        smoothed = smoothed + (relaxation / 6.0) * (right_side - apply_stencil(smoothed))
    residual = right_side - apply_stencil(smoothed)
    coarse_rhs = restrict_axis(restrict_axis(restrict_axis(residual, 0), 1), 2)
    correction = jnp.zeros_like(coarse_rhs)
    for sweep_num in range(COARSE_SWEEPS):
        correction = correction + (relaxation / 1.5) * (coarse_rhs - 0.25 * apply_stencil(correction))
    fine_corr = prolong_axis(prolong_axis(prolong_axis(correction, 0), 1), 2)
    return smoothed + fine_corr
```

```python
import functools

import jax
import jax.numpy as jnp
from jax import lax
from jax.experimental import pallas as pl
from jax.experimental.pallas import tpu as pltpu
from jax.sharding import PartitionSpec as P

MESH = pl.DeviceIdType.MESH
F32 = jnp.float32
BF16 = jnp.bfloat16
SEVENTH = 1.0 / 7.0
AXES = ("gx", "gy", "gz")
SEND = {-1: (3, 4), 0: (3, 34), 1: (32, 5)}
LAND = {-1: 35, 0: 3, 1: 0}
TSEND = {-1: (0, 1), 0: (0, 3), 1: (2, 1)}
TLAND = {-1: 2, 0: 0, 1: 0}
XY = [(dx, dy) for dx in (-1, 0, 1) for dy in (-1, 0, 1)]
XY8 = [d for d in XY if d != (0, 0)]


def split3(v):
    hi = v.astype(BF16)
    rest = v - hi.astype(F32)
    mid = rest.astype(BF16)
    lo = (rest - mid.astype(F32)).astype(BF16)
    return hi, mid, lo


def dot3(v, weights):
    parts = [jnp.dot(p, weights, preferred_element_type=F32) for p in split3(v)]
    return (parts[2] + parts[1]) + parts[0]


def kernel(s_in, b_in, out, *scratch):
    (u0, u1, u2, bv, ez, zr, at, qb, wr, wp, gm, gs, lh, ls, kc, g2, ca, cb, fz, wt) = scratch[:20]
    rm = scratch[20:28]
    rl = scratch[28:36]
    rz = scratch[36:45]
    load_sem, out_sem, f_send, f_recv, m_send, m_recv, l_send, l_recv, z_send, z_recv = scratch[45:]

    gx, gy, gz = (lax.axis_index(a) for a in AXES)
    nx, ny, nz = (lax.axis_size(a) for a in AXES)
    me = {"gx": gx, "gy": gy, "gz": gz}
    size = {"gx": nx, "gy": ny, "gz": nz}

    def has(axis, d):
        if d == 0:
            return True
        return me[axis] < size[axis] - 1 if d > 0 else me[axis] > 0

    def has_all(dx, dy, dz):
        ok = None
        for axis, d in zip(AXES, (dx, dy, dz)):
            if d:
                here = has(axis, d)
                ok = here if ok is None else jnp.logical_and(ok, here)
        return ok

    def target(dx, dy, dz):
        return {a: me[a] + d for a, d in zip(AXES, (dx, dy, dz))}

    loads = []
    for h in range(2):
        lanes = pl.ds(128 * h, 128)
        loads.append(pltpu.make_async_copy(s_in.at[:, :, lanes], u0.at[pl.ds(1, 64), h, pl.ds(8, 64), :], load_sem.at[h]))
    for h in range(2):
        lanes = pl.ds(128 * h, 128)
        loads.append(pltpu.make_async_copy(b_in.at[:, :, lanes], bv.at[pl.ds(2, 64), h], load_sem.at[2 + h]))
    for c in loads:
        c.start()

    barrier = pltpu.get_barrier_semaphore()
    count = jnp.int32(0)
    for axis in AXES:
        for d in (-1, 1):
            ok = has(axis, d)
            count = count + ok.astype(jnp.int32)

            @pl.when(ok)
            def _():
                pl.semaphore_signal(barrier, inc=1, device_id={axis: me[axis] + d}, device_id_type=MESH)

    lane = lax.broadcasted_iota(jnp.int32, (64, 128), 1)
    first = lane == 0
    last = lane == 127
    group = lax.rem((lane + 1) // 2, 64)

    zplane = jnp.zeros((2, 80, 128), F32)
    zrow = jnp.zeros((1, 128), F32)

    @pl.when(gx == 0)
    def _():
        u0[0] = zplane
        u1[0] = zplane

    @pl.when(gx == nx - 1)
    def _():
        u0[65] = zplane
        u1[65] = zplane

    def zero_rows(row):
        def body(x, _):
            for h in range(2):
                u0[x, h, pl.ds(row, 1), :] = zrow
                u1[x, h, pl.ds(row, 1), :] = zrow
            return 0

        lax.fori_loop(1, 65, body, 0)

    @pl.when(gy == 0)
    def _():
        zero_rows(7)

    @pl.when(gy == ny - 1)
    def _():
        zero_rows(72)

    @pl.when(gz == 0)
    def _():
        zr[0, 0] = jnp.zeros((64, 128), F32)
        zr[1, 0] = jnp.zeros((64, 128), F32)

    @pl.when(gz == nz - 1)
    def _():
        zr[0, 1] = jnp.zeros((64, 128), F32)
        zr[1, 1] = jnp.zeros((64, 128), F32)

    for p in (0, 1, 2, 67, 68, 69, 70):
        u2[p] = zplane
    for p in (0, 1, 66, 67, 68):
        bv[p] = jnp.zeros((2, 64, 128), F32)
    at[...] = jnp.zeros(at.shape, F32)

    def coarse_of(column):
        inner = column - 128
        return jnp.where(column < 128, column, jnp.where(inner >= 64, inner - 128, inner + 128))

    zi = lax.broadcasted_iota(jnp.int32, (256, 256), 0)
    kci = coarse_of(lax.broadcasted_iota(jnp.int32, (256, 256), 1))
    d = zi - 2 * kci
    zero = jnp.zeros((256, 256), F32)
    plain = jnp.where(d == 1, -2.0, jnp.where((d == 0) | (d == 2), -1.0, zero))
    topz = (gz == nz - 1).astype(F32)
    edge = jnp.where((zi == 255) & (kci == 127), topz, zero)
    around = jnp.where((d >= 0) & (d <= 2), 2.0, jnp.where((d == -1) | (d == 3), 1.0, zero)) - edge
    wr[pl.ds(0, 256), :] = plain.astype(BF16)
    wr[pl.ds(256, 256), :] = around.astype(BF16)
    kr = coarse_of(lax.broadcasted_iota(jnp.int32, (256, 256), 0))
    d = lax.broadcasted_iota(jnp.int32, (256, 256), 1) - 2 * kr
    wp[...] = jnp.where(d == 1, 1.0, jnp.where((d == 0) | (d == 2), 0.5, zero)).astype(BF16)

    r40 = lax.broadcasted_iota(jnp.int32, (40, 128), 0)
    l40 = lax.broadcasted_iota(jnp.int32, (40, 128), 1)
    zero40 = jnp.zeros((40, 128), F32)
    low_y = jnp.where(gy > 0, 0, 4)
    high_y = jnp.where(gy < ny - 1, 40, 36)
    low_z = jnp.where(gz > 0, 124, 128)
    high_z = jnp.where(gz < nz - 1, 4, 0)
    rows_in = jnp.where((r40 >= low_y) & (r40 < high_y), SEVENTH, zero40)
    kc[0] = rows_in
    kc[1] = jnp.where((l40 >= low_z) | (l40 < high_z), rows_in, zero40)
    topy = (gy == ny - 1).astype(F32)
    kc[2] = 0.5 - jnp.where(r40 == 35, 0.25 * topy, zero40)

    def faces(r, u):
        x_in = (slice(None), pl.ds(8, 64), slice(None))
        xs = pl.ds(1, 64)
        every = slice(None)
        plan = [
            ("gx", 1, u.at[(64,) + x_in], u.at[(0,) + x_in]),
            ("gx", -1, u.at[(1,) + x_in], u.at[(65,) + x_in]),
            ("gy", 1, u.at[xs, every, pl.ds(71, 1), every], u.at[xs, every, pl.ds(7, 1), every]),
            ("gy", -1, u.at[xs, every, pl.ds(8, 1), every], u.at[xs, every, pl.ds(72, 1), every]),
            ("gz", 1, ez.at[r], zr.at[r, 0]),
            ("gz", -1, ez.at[r], zr.at[r, 1]),
        ]
        done = []
        for k, (axis, dd, src, dst) in enumerate(plan):
            copy = pltpu.make_async_remote_copy(
                src_ref=src, dst_ref=dst, send_sem=f_send.at[r, k], recv_sem=f_recv.at[r, k],
                device_id={axis: me[axis] + dd}, device_id_type=MESH,
            )
            done.append((axis, dd, copy))
        return done

    def start(copies):
        for axis, dd, copy in copies:
            pl.when(has(axis, dd))(copy.start)

    def arrive(copies):
        for axis, dd, copy in copies:
            pl.when(has(axis, -dd))(copy.wait_recv)

    def sent(copies):
        for axis, dd, copy in copies:
            pl.when(has(axis, dd))(copy.wait_send)

    round0, round1 = faces(0, u0), faces(1, u1)

    loads[0].wait()
    loads[1].wait()
    pl.semaphore_wait(barrier, count)
    start(round0[:4])

    def pack_face(low, high, x, packed):
        both = jnp.where(first, low, high)
        return jnp.where(group == x, pltpu.roll(both, 2 * x, 1), packed)

    def pack(x, packed):
        return pack_face(u0[x + 1, 0, pl.ds(8, 64), :], u0[x + 1, 1, pl.ds(8, 64), :], x, packed)

    ez[0] = lax.fori_loop(0, 64, pack, jnp.zeros((64, 128), F32), unroll=4)
    start(round0[4:])

    def sweep(r, u, off, v, voff):
        even = lax.rem(lane, 2) == 0
        halo = jnp.where(even, pltpu.roll(zr[r, 0], 1, 1), pltpu.roll(zr[r, 1], 127, 1))
        zr[r, 0] = halo

        def body(x, packed):
            side = pltpu.roll(zr[r, 0], lax.rem(128 - 2 * x, 128), 1)
            c = [u[x + off, h, pl.ds(8, 64), :] for h in range(2)]
            right = [pltpu.roll(c[h], 1, 1) for h in range(2)]
            left = [pltpu.roll(c[h], 127, 1) for h in range(2)]
            below = [jnp.where(first, side, right[0]), jnp.where(first, right[0], right[1])]
            above = [jnp.where(last, left[1], left[0]), jnp.where(last, side, left[1])]
            new = []
            for h in range(2):
                total = u[x + off - 1, h, pl.ds(8, 64), :] + u[x + off + 1, h, pl.ds(8, 64), :]
                total = total + (u[x + off, h, pl.ds(7, 64), :] + u[x + off, h, pl.ds(9, 64), :])
                total = total + (c[h] + bv[x + 2, h])
                total = (total + (below[h] + above[h])) * SEVENTH
                v[x + voff, h, pl.ds(8, 64), :] = total
                new.append(total)
            if r == 0:
                packed = pack_face(new[0], new[1], x, packed)
            return packed

        init = jnp.zeros((64, 128), F32) if r == 0 else jnp.int32(0)
        return lax.fori_loop(0, 64, body, init, unroll=2)

    loads[2].wait()
    loads[3].wait()
    arrive(round0)
    ez[1] = sweep(0, u0, 1, u1, 1)
    start(round1)
    arrive(round1)
    sweep(1, u1, 1, u2, 3)

    topx = gx == nx - 1

    def restrict(i, _):
        slot = lax.rem(i, 2)
        mid = jnp.where(jnp.logical_and(topx, i == 32), 2.75, 2.5).astype(F32)
        for h in range(2):
            w = [u2[2 * i + k, h, pl.ds(8, 64), :] for k in range(5)]
            b = [bv[2 * i + k, h] for k in range(3)]
            beside = w[1] + w[3]
            at[slot, h, pl.ds(16, 64), :] = 0.25 * beside + 0.5 * w[2]
            load = 0.25 * (b[0] + b[2]) + 0.5 * b[1]
            at[slot, 2 + h, pl.ds(16, 64), :] = (beside - 0.25 * (w[0] + w[4])) + (mid * w[2] - load)
        for h in range(2):
            a1 = [at[slot, h, pl.ds(8 + o, 40, stride=2), :] for o in (-1, 0, 1, 2, 3)]
            a2 = [at[slot, 2 + h, pl.ds(8 + o, 40, stride=2), :] for o in (0, 1, 2)]
            beside = a1[1] + a1[3]
            main = 0.25 * (a2[0] + a2[2]) + 0.5 * a2[1]
            main = main - (0.25 * (a1[0] + a1[4]) + 0.5 * beside) - kc[2] * a1[2]
            qb[i, :, pl.ds(128 * h, 128)] = main
            qb[i, :, pl.ds(256 + 128 * h, 128)] = 0.25 * beside + 0.5 * a1[2]
        return 0

    lax.fori_loop(0, 34, restrict, 0, unroll=2)

    gm[...] = jnp.zeros(gm.shape, F32)
    gs[...] = jnp.zeros(gs.shape, F32)

    def restrict_z(n, _):
        i = 17 * n
        got = dot3(qb[pl.ds(i, 17)].reshape(680, 512), wr[...])
        main = got[:, :128].reshape(17, 40, 128)
        gm[pl.ds(i + 3, 17)] = main
        gs[pl.ds(i + 3, 17)] = main
        g2[pl.ds(i + 3, 17), 1] = got[:, 128:].reshape(17, 40, 128)
        return 0

    lax.fori_loop(0, 2, restrict_z, 0)

    edge40 = l40 >= 124
    oct40 = l40 // 8
    for t, (lo, hi) in enumerate(((3, 16), (16, 32), (32, 37))):

        def pack_ends(p, ends):
            main, halo = gm[p], g2[p, 1]
            q = p - 16 * t
            shift = lax.rem(8 * q + 4, 128)
            here = oct40 == q
            return (
                jnp.where(here, pltpu.roll(jnp.where(edge40, halo, main), shift, 1), ends[0]),
                jnp.where(here, pltpu.roll(jnp.where(edge40, main, halo), shift, 1), ends[1]),
            )

        ends = lax.fori_loop(lo, hi, pack_ends, (zero40, zero40))
        for k in range(2):
            lh[k, t] = ends[k]
            ls[k, t] = ends[k]

    messages = []
    for n, (dx, dy) in enumerate(XY8):
        (xa, xn), (ya, yn) = SEND[dx], SEND[dy]
        (ta, tn) = TSEND[dx]
        to = target(dx, dy, 0)
        messages.append((dx, dy, 0, pltpu.make_async_remote_copy(
            src_ref=gm.at[pl.ds(xa, xn), pl.ds(ya, yn), :], dst_ref=rm[n],
            send_sem=m_send.at[n], recv_sem=m_recv.at[n], device_id=to, device_id_type=MESH)))
        messages.append((dx, dy, 0, pltpu.make_async_remote_copy(
            src_ref=lh.at[:, pl.ds(ta, tn), pl.ds(ya, yn), :], dst_ref=rl[n],
            send_sem=l_send.at[n], recv_sem=l_recv.at[n], device_id=to, device_id_type=MESH)))
    for n, (dx, dy) in enumerate(XY):
        ya, yn = SEND[dy]
        ta, tn = TSEND[dx]
        for dz in (-1, 1):
            end = 1 if dz > 0 else 0
            messages.append((dx, dy, dz, pltpu.make_async_remote_copy(
                src_ref=lh.at[end, pl.ds(ta, tn), pl.ds(ya, yn), :], dst_ref=rz[n].at[1 - end],
                send_sem=z_send.at[n, end], recv_sem=z_recv.at[n, end],
                device_id=target(dx, dy, dz), device_id_type=MESH)))
    for dx, dy, dz, copy in messages:
        pl.when(has_all(dx, dy, dz))(copy.start)

    for n, (dx, dy, dz, copy) in enumerate(messages):
        xn, yn, tn = SEND[dx][1], SEND[dy][1], TSEND[dx][1]
        xl, yl, tl = LAND[dx], LAND[dy], TLAND[dx]

        @pl.when(has_all(-dx, -dy, -dz))
        def _():
            copy.wait_recv()
            rows = pl.ds(yl, yn)
            if dz == 0 and n % 2 == 0:
                src = rm[n // 2]

                def add(p, _):
                    gs[xl + p, rows, :] = gs[xl + p, rows, :] + src[p]
                    return 0

                lax.fori_loop(0, xn, add, 0)
            elif dz == 0:
                src = rl[n // 2]
                for k in range(2):
                    for t in range(tn):
                        ls[k, tl + t, rows, :] = ls[k, tl + t, rows, :] + src[k, t]
            else:
                k = 0 if dz > 0 else 1
                src = rz[(n - 16) // 2]
                for t in range(tn):
                    ls[k, tl + t, rows, :] = ls[k, tl + t, rows, :] + src[k, t]

    begin40 = l40 < 4
    zpad = jnp.zeros((40, 2, 8, 128), F32)
    for c in (ca, cb):
        c[:, :, pl.ds(0, 8), :] = zpad
        c[:, :, pl.ds(48, 8), :] = zpad

    def assemble(p, _):
        t = p // 16
        q = p - 16 * t
        shift = lax.rem(252 - 8 * q, 128)
        low = pltpu.roll(ls[0, t], shift, 1)
        high = pltpu.roll(ls[1, t], shift, 1)
        main = jnp.where(begin40, low, jnp.where(edge40, high, gs[p]))
        halo = jnp.where(begin40, high, jnp.where(edge40, low, zero40))
        g2[p, 0] = main
        g2[p, 1] = halo
        ca[p, 0, pl.ds(8, 40), :] = main * kc[0]
        ca[p, 1, pl.ds(8, 40), :] = halo * kc[1]
        return 0

    lax.fori_loop(0, 40, assemble, 0, unroll=2)

    zc = jnp.zeros((2, 40, 128), F32)

    def clip(c):
        @pl.when(gx == 0)
        def _():
            for p in range(4):
                c[p, :, pl.ds(8, 40), :] = zc

        @pl.when(gx == nx - 1)
        def _():
            for p in range(36, 40):
                c[p, :, pl.ds(8, 40), :] = zc

    first40 = l40 == 0
    last40 = l40 == 127

    def coarse_sweep(c, v, lo, hi):
        def body(p, _):
            own = [c[p, h, pl.ds(8, 40), :] for h in range(2)]
            right = [pltpu.roll(own[h], 1, 1) for h in range(2)]
            left = [pltpu.roll(own[h], 127, 1) for h in range(2)]
            for h in range(2):
                total = c[p - 1, h, pl.ds(8, 40), :] + c[p + 1, h, pl.ds(8, 40), :]
                total = total + (c[p, h, pl.ds(7, 40), :] + c[p, h, pl.ds(9, 40), :])
                total = total + (own[h] + g2[p, h])
                total = total + jnp.where(first40, right[1 - h], right[h])
                total = total + jnp.where(last40, left[1 - h], left[h])
                v[p, h, pl.ds(8, 40), :] = total * kc[h]
            return 0

        lax.fori_loop(lo, hi, body, 0, unroll=2)
        clip(v)

    clip(ca)
    coarse_sweep(ca, cb, 1, 39)
    coarse_sweep(cb, ca, 2, 38)
    coarse_sweep(ca, cb, 3, 37)

    def prolong_z(n, _):
        i = 11 * n
        block = [cb[pl.ds(3 + i, 11), h, pl.ds(8, 40), :].reshape(440, 128) for h in range(2)]
        got = dot3(jnp.concatenate(block, axis=1), wp[...])
        for h in range(2):
            fz[pl.ds(i, 11), h] = got[:, 128 * h : 128 * h + 128].reshape(11, 40, 128)
        return 0

    lax.fori_loop(0, 3, prolong_z, 0)

    def prolong_y(j, slot):
        for h in range(2):
            here = fz[j, h, pl.ds(4, 32), :]
            wt[slot, h, pl.ds(0, 32, stride=2), :] = 0.5 * (fz[j, h, pl.ds(3, 32), :] + here)
            wt[slot, h, pl.ds(1, 32, stride=2), :] = here

    prolong_y(0, 0)

    def outgoing(x, n, h):
        return pltpu.make_async_copy(
            u2.at[pl.ds(3 + x, n), h, pl.ds(8, 64), :], out.at[pl.ds(x, n), :, pl.ds(128 * h, 128)], out_sem.at[h])

    def finish(i, _):
        slot = lax.rem(i + 1, 2)
        prolong_y(i + 1, slot)
        for h in range(2):
            here = wt[slot, h]
            mean = 0.5 * (wt[1 - slot, h] + here)
            u2[2 * i + 3, h, pl.ds(8, 64), :] = u2[2 * i + 3, h, pl.ds(8, 64), :] + mean
            u2[2 * i + 4, h, pl.ds(8, 64), :] = u2[2 * i + 4, h, pl.ds(8, 64), :] + here
        for h in range(2):
            outgoing(2 * i, 2, h).start()
        return 0

    lax.fori_loop(0, 32, finish, 0)
    for h in range(2):
        outgoing(0, 64, h).wait()
    sent(round0)
    sent(round1)
    for dx, dy, dz, copy in messages:
        pl.when(has_all(dx, dy, dz))(copy.wait_send)


def on_device(start_field, right_side):
    v = pltpu.VMEM
    scratch = [
        v((66, 2, 80, 128), F32), v((66, 2, 80, 128), F32), v((71, 2, 80, 128), F32),
        v((69, 2, 64, 128), F32), v((2, 64, 128), F32), v((2, 2, 64, 128), F32),
        v((2, 4, 96, 128), F32), v((34, 40, 512), F32), v((512, 256), BF16), v((256, 256), BF16),
        v((40, 40, 128), F32), v((40, 40, 128), F32), v((2, 3, 40, 128), F32), v((2, 3, 40, 128), F32),
        v((3, 40, 128), F32), v((40, 2, 40, 128), F32), v((40, 2, 56, 128), F32), v((40, 2, 56, 128), F32),
        v((33, 2, 40, 128), F32), v((2, 2, 64, 128), F32),
    ]
    scratch += [v((SEND[dx][1], SEND[dy][1], 128), F32) for dx, dy in XY8]
    scratch += [v((2, TSEND[dx][1], SEND[dy][1], 128), F32) for dx, dy in XY8]
    scratch += [v((2, TSEND[dx][1], SEND[dy][1], 128), F32) for dx, dy in XY]
    dma = pltpu.SemaphoreType.DMA
    scratch += [dma((4,)), dma((2,)), dma((2, 6)), dma((2, 6)), dma((8,)), dma((8,)), dma((8,)), dma((8,)),
                dma((9, 2)), dma((9, 2))]
    anywhere = pl.BlockSpec(memory_space=pl.ANY)
    return pl.pallas_call(
        kernel,
        out_shape=jax.ShapeDtypeStruct(start_field.shape, F32),
        in_specs=[anywhere, anywhere],
        out_specs=anywhere,
        scratch_shapes=scratch,
        compiler_params=pltpu.CompilerParams(
            collective_id=0, has_side_effects=True, vmem_limit_bytes=60 * 1024 * 1024),
    )(start_field, right_side)


def solution(mesh):
    placed = P("gx", "gy", "gz")
    return jax.shard_map(on_device, mesh=mesh, in_specs=(placed, placed), out_specs=placed, check_vma=False)
```

```python
import functools

import jax
import jax.numpy as jnp
from jax import lax
from jax.experimental import pallas as pl
from jax.experimental.pallas import tpu as pltpu
from jax.sharding import PartitionSpec as P

MESH = pl.DeviceIdType.MESH
F32 = jnp.float32
BF16 = jnp.bfloat16
SEVENTH = 1.0 / 7.0
UP, US, UE, UA, UR, UF = 8, 8, 8, 8, 2, 2
UC = (8, 6, 7)
AXES = ("gx", "gy", "gz")
SEND = {-1: (3, 4), 0: (3, 34), 1: (32, 5)}
LAND = {-1: 35, 0: 3, 1: 0}
TSEND = {-1: (0, 1), 0: (0, 3), 1: (2, 1)}
TLAND = {-1: 2, 0: 0, 1: 0}
XY = [(dx, dy) for dx in (-1, 0, 1) for dy in (-1, 0, 1)]
XY8 = [d for d in XY if d != (0, 0)]


def split3(v):
    hi = v.astype(BF16)
    rest = v - hi.astype(F32)
    mid = rest.astype(BF16)
    lo = (rest - mid.astype(F32)).astype(BF16)
    return hi, mid, lo


def dot3(v, weights):
    parts = [jnp.dot(p, weights, preferred_element_type=F32) for p in split3(v)]
    return (parts[2] + parts[1]) + parts[0]


def kernel(s_in, b_in, u2, fz, *scratch):
    (u0, u1, bv, ez, zr, at, qb, wr, wp, gm, gs, lh, ls, kc, g2, ca, cb) = scratch[:17]
    rm = scratch[17:25]
    rl = scratch[25:33]
    rz = scratch[33:42]
    load_sem, f_send, f_recv, m_send, m_recv, l_send, l_recv, z_send, z_recv = scratch[42:]

    gx, gy, gz = (lax.axis_index(a) for a in AXES)
    nx, ny, nz = (lax.axis_size(a) for a in AXES)
    me = {"gx": gx, "gy": gy, "gz": gz}
    size = {"gx": nx, "gy": ny, "gz": nz}

    def has(axis, d):
        if d == 0:
            return True
        return me[axis] < size[axis] - 1 if d > 0 else me[axis] > 0

    def has_all(dx, dy, dz):
        ok = None
        for axis, d in zip(AXES, (dx, dy, dz)):
            if d:
                here = has(axis, d)
                ok = here if ok is None else jnp.logical_and(ok, here)
        return ok

    def target(dx, dy, dz):
        return {a: me[a] + d for a, d in zip(AXES, (dx, dy, dz))}

    loads = []
    for h in range(2):
        lanes = pl.ds(128 * h, 128)
        loads.append(pltpu.make_async_copy(s_in.at[:, :, lanes], u0.at[pl.ds(1, 64), h, pl.ds(8, 64), :], load_sem.at[h]))
    for h in range(2):
        lanes = pl.ds(128 * h, 128)
        loads.append(pltpu.make_async_copy(b_in.at[:, :, lanes], bv.at[pl.ds(2, 64), h], load_sem.at[2 + h]))
    for c in loads:
        c.start()

    barrier = pltpu.get_barrier_semaphore()
    count = jnp.int32(0)
    for axis in AXES:
        for d in (-1, 1):
            ok = has(axis, d)
            count = count + ok.astype(jnp.int32)

            @pl.when(ok)
            def _():
                pl.semaphore_signal(barrier, inc=1, device_id={axis: me[axis] + d}, device_id_type=MESH)

    lane = lax.broadcasted_iota(jnp.int32, (64, 128), 1)
    first = lane == 0
    last = lane == 127
    group = lax.rem((lane + 1) // 2, 64)

    zplane = jnp.zeros((2, 80, 128), F32)
    zrow = jnp.zeros((1, 128), F32)

    @pl.when(gx == 0)
    def _():
        u0[0] = zplane
        u1[0] = zplane

    @pl.when(gx == nx - 1)
    def _():
        u0[65] = zplane
        u1[65] = zplane

    def zero_rows(row):
        def body(x, _):
            for h in range(2):
                u0[x, h, pl.ds(row, 1), :] = zrow
                u1[x, h, pl.ds(row, 1), :] = zrow
            return 0

        lax.fori_loop(1, 65, body, 0)

    @pl.when(gy == 0)
    def _():
        zero_rows(7)

    @pl.when(gy == ny - 1)
    def _():
        zero_rows(72)

    @pl.when(gz == 0)
    def _():
        zr[0, 0] = jnp.zeros((64, 128), F32)
        zr[1, 0] = jnp.zeros((64, 128), F32)

    @pl.when(gz == nz - 1)
    def _():
        zr[0, 1] = jnp.zeros((64, 128), F32)
        zr[1, 1] = jnp.zeros((64, 128), F32)

    for p in (0, 1, 2, 67, 68, 69, 70):
        u2[p] = zplane
    for p in (0, 1, 66, 67, 68):
        bv[p] = jnp.zeros((2, 64, 128), F32)
    at[...] = jnp.zeros(at.shape, F32)

    def coarse_of(column):
        inner = column - 128
        return jnp.where(column < 128, column, jnp.where(inner >= 64, inner - 128, inner + 128))

    zi = lax.broadcasted_iota(jnp.int32, (256, 256), 0)
    kci = coarse_of(lax.broadcasted_iota(jnp.int32, (256, 256), 1))
    d = zi - 2 * kci
    zero = jnp.zeros((256, 256), F32)
    plain = jnp.where(d == 1, -2.0, jnp.where((d == 0) | (d == 2), -1.0, zero))
    topz = (gz == nz - 1).astype(F32)
    edge = jnp.where((zi == 255) & (kci == 127), topz, zero)
    around = jnp.where((d >= 0) & (d <= 2), 2.0, jnp.where((d == -1) | (d == 3), 1.0, zero)) - edge
    wr[pl.ds(0, 256), :] = plain.astype(BF16)
    wr[pl.ds(256, 256), :] = around.astype(BF16)
    kr = coarse_of(lax.broadcasted_iota(jnp.int32, (256, 256), 0))
    d = lax.broadcasted_iota(jnp.int32, (256, 256), 1) - 2 * kr
    wp[...] = jnp.where(d == 1, 1.0, jnp.where((d == 0) | (d == 2), 0.5, zero)).astype(BF16)

    r40 = lax.broadcasted_iota(jnp.int32, (40, 128), 0)
    l40 = lax.broadcasted_iota(jnp.int32, (40, 128), 1)
    zero40 = jnp.zeros((40, 128), F32)
    low_y = jnp.where(gy > 0, 0, 4)
    high_y = jnp.where(gy < ny - 1, 40, 36)
    low_z = jnp.where(gz > 0, 124, 128)
    high_z = jnp.where(gz < nz - 1, 4, 0)
    rows_in = jnp.where((r40 >= low_y) & (r40 < high_y), SEVENTH, zero40)
    kc[0] = rows_in
    kc[1] = jnp.where((l40 >= low_z) | (l40 < high_z), rows_in, zero40)
    topy = (gy == ny - 1).astype(F32)
    kc[2] = 0.5 - jnp.where(r40 == 35, 0.25 * topy, zero40)

    def faces(r, u):
        x_in = (slice(None), pl.ds(8, 64), slice(None))
        xs = pl.ds(1, 64)
        every = slice(None)
        plan = [
            ("gx", 1, u.at[(64,) + x_in], u.at[(0,) + x_in]),
            ("gx", -1, u.at[(1,) + x_in], u.at[(65,) + x_in]),
            ("gy", 1, u.at[xs, every, pl.ds(71, 1), every], u.at[xs, every, pl.ds(7, 1), every]),
            ("gy", -1, u.at[xs, every, pl.ds(8, 1), every], u.at[xs, every, pl.ds(72, 1), every]),
            ("gz", 1, ez.at[r], zr.at[r, 0]),
            ("gz", -1, ez.at[r], zr.at[r, 1]),
        ]
        done = []
        for k, (axis, dd, src, dst) in enumerate(plan):
            copy = pltpu.make_async_remote_copy(
                src_ref=src, dst_ref=dst, send_sem=f_send.at[r, k], recv_sem=f_recv.at[r, k],
                device_id={axis: me[axis] + dd}, device_id_type=MESH,
            )
            done.append((axis, dd, copy))
        return done

    def start(copies):
        for axis, dd, copy in copies:
            pl.when(has(axis, dd))(copy.start)

    def arrive(copies):
        for axis, dd, copy in copies:
            pl.when(has(axis, -dd))(copy.wait_recv)

    def sent(copies):
        for axis, dd, copy in copies:
            pl.when(has(axis, dd))(copy.wait_send)

    round0, round1 = faces(0, u0), faces(1, u1)

    loads[0].wait()
    loads[1].wait()
    pl.semaphore_wait(barrier, count)
    start(round0[:4])

    def pack_face(low, high, x, packed):
        both = jnp.where(first, low, high)
        return jnp.where(group == x, pltpu.roll(both, 2 * x, 1), packed)

    def pack(x, packed):
        return pack_face(u0[x + 1, 0, pl.ds(8, 64), :], u0[x + 1, 1, pl.ds(8, 64), :], x, packed)

    ez[0] = lax.fori_loop(0, 64, pack, jnp.zeros((64, 128), F32), unroll=UP)
    start(round0[4:])

    def sweep(r, u, off, v, voff):
        even = lax.rem(lane, 2) == 0
        halo = jnp.where(even, pltpu.roll(zr[r, 0], 1, 1), pltpu.roll(zr[r, 1], 127, 1))
        zr[r, 0] = halo

        def body(x, packed):
            side = pltpu.roll(zr[r, 0], lax.rem(128 - 2 * x, 128), 1)
            c = [u[x + off, h, pl.ds(8, 64), :] for h in range(2)]
            right = [pltpu.roll(c[h], 1, 1) for h in range(2)]
            left = [pltpu.roll(c[h], 127, 1) for h in range(2)]
            below = [jnp.where(first, side, right[0]), jnp.where(first, right[0], right[1])]
            above = [jnp.where(last, left[1], left[0]), jnp.where(last, side, left[1])]
            new = []
            for h in range(2):
                total = u[x + off - 1, h, pl.ds(8, 64), :] + u[x + off + 1, h, pl.ds(8, 64), :]
                total = total + (u[x + off, h, pl.ds(7, 64), :] + u[x + off, h, pl.ds(9, 64), :])
                total = total + (c[h] + bv[x + 2, h])
                total = (total + (below[h] + above[h])) * SEVENTH
                v[x + voff, h, pl.ds(8, 64), :] = total
                new.append(total)
            if r == 0:
                packed = pack_face(new[0], new[1], x, packed)
            return packed

        init = jnp.zeros((64, 128), F32) if r == 0 else jnp.int32(0)
        return lax.fori_loop(0, 64, body, init, unroll=US)

    loads[2].wait()
    loads[3].wait()
    arrive(round0)
    ez[1] = sweep(0, u0, 1, u1, 1)
    start(round1)
    arrive(round1)
    sweep(1, u1, 1, u2, 3)

    topx = gx == nx - 1

    def restrict(i, _):
        slot = lax.rem(i, 2)
        mid = jnp.where(jnp.logical_and(topx, i == 32), 2.75, 2.5).astype(F32)
        for h in range(2):
            w = [u2[2 * i + k, h, pl.ds(8, 64), :] for k in range(5)]
            b = [bv[2 * i + k, h] for k in range(3)]
            beside = w[1] + w[3]
            at[slot, h, pl.ds(16, 64), :] = 0.25 * beside + 0.5 * w[2]
            load = 0.25 * (b[0] + b[2]) + 0.5 * b[1]
            at[slot, 2 + h, pl.ds(16, 64), :] = (beside - 0.25 * (w[0] + w[4])) + (mid * w[2] - load)
        for h in range(2):
            a1 = [at[slot, h, pl.ds(8 + o, 40, stride=2), :] for o in (-1, 0, 1, 2, 3)]
            a2 = [at[slot, 2 + h, pl.ds(8 + o, 40, stride=2), :] for o in (0, 1, 2)]
            beside = a1[1] + a1[3]
            main = 0.25 * (a2[0] + a2[2]) + 0.5 * a2[1]
            main = main - (0.25 * (a1[0] + a1[4]) + 0.5 * beside) - kc[2] * a1[2]
            qb[i, :, pl.ds(128 * h, 128)] = main
            qb[i, :, pl.ds(256 + 128 * h, 128)] = 0.25 * beside + 0.5 * a1[2]
        return 0

    lax.fori_loop(0, 34, restrict, 0, unroll=UR)

    gm[...] = jnp.zeros(gm.shape, F32)
    for p in (0, 1, 2, 37, 38, 39):
        g2[p, 1] = zero40
    gs[...] = jnp.zeros(gs.shape, F32)

    def restrict_z(n, _):
        i = 17 * n
        got = dot3(qb[pl.ds(i, 17)].reshape(680, 512), wr[...])
        main = got[:, :128].reshape(17, 40, 128)
        gm[pl.ds(i + 3, 17)] = main
        gs[pl.ds(i + 3, 17)] = main
        g2[pl.ds(i + 3, 17), 1] = got[:, 128:].reshape(17, 40, 128)
        return 0

    lax.fori_loop(0, 2, restrict_z, 0)

    edge40 = l40 >= 124
    oct40 = l40 // 8
    for t, (lo, hi) in enumerate(((0, 16), (16, 32), (32, 40))):

        def pack_ends(p, ends):
            main, halo = gm[p], g2[p, 1]
            q = p - 16 * t
            shift = lax.rem(8 * q + 4, 128)
            here = oct40 == q
            return (
                jnp.where(here, pltpu.roll(jnp.where(edge40, halo, main), shift, 1), ends[0]),
                jnp.where(here, pltpu.roll(jnp.where(edge40, main, halo), shift, 1), ends[1]),
            )

        ends = lax.fori_loop(lo, hi, pack_ends, (zero40, zero40), unroll=UE)
        for k in range(2):
            lh[k, t] = ends[k]
            ls[k, t] = ends[k]

    messages = []
    for n, (dx, dy) in enumerate(XY8):
        (xa, xn), (ya, yn) = SEND[dx], SEND[dy]
        (ta, tn) = TSEND[dx]
        to = target(dx, dy, 0)
        messages.append((dx, dy, 0, pltpu.make_async_remote_copy(
            src_ref=gm.at[pl.ds(xa, xn), pl.ds(ya, yn), :], dst_ref=rm[n],
            send_sem=m_send.at[n], recv_sem=m_recv.at[n], device_id=to, device_id_type=MESH)))
        messages.append((dx, dy, 0, pltpu.make_async_remote_copy(
            src_ref=lh.at[:, pl.ds(ta, tn), pl.ds(ya, yn), :], dst_ref=rl[n],
            send_sem=l_send.at[n], recv_sem=l_recv.at[n], device_id=to, device_id_type=MESH)))
    for n, (dx, dy) in enumerate(XY):
        ya, yn = SEND[dy]
        ta, tn = TSEND[dx]
        for dz in (-1, 1):
            end = 1 if dz > 0 else 0
            messages.append((dx, dy, dz, pltpu.make_async_remote_copy(
                src_ref=lh.at[end, pl.ds(ta, tn), pl.ds(ya, yn), :], dst_ref=rz[n].at[1 - end],
                send_sem=z_send.at[n, end], recv_sem=z_recv.at[n, end],
                device_id=target(dx, dy, dz), device_id_type=MESH)))
    for dx, dy, dz, copy in messages:
        pl.when(has_all(dx, dy, dz))(copy.start)

    for n, (dx, dy, dz, copy) in enumerate(messages):
        xn, yn, tn = SEND[dx][1], SEND[dy][1], TSEND[dx][1]
        xl, yl, tl = LAND[dx], LAND[dy], TLAND[dx]

        @pl.when(has_all(-dx, -dy, -dz))
        def _():
            copy.wait_recv()
            rows = pl.ds(yl, yn)
            if dz == 0 and n % 2 == 0:
                src = rm[n // 2]

                def add(p, _):
                    gs[xl + p, rows, :] = gs[xl + p, rows, :] + src[p]
                    return 0

                lax.fori_loop(0, xn, add, 0)
            elif dz == 0:
                src = rl[n // 2]
                for k in range(2):
                    for t in range(tn):
                        ls[k, tl + t, rows, :] = ls[k, tl + t, rows, :] + src[k, t]
            else:
                k = 0 if dz > 0 else 1
                src = rz[(n - 16) // 2]
                for t in range(tn):
                    ls[k, tl + t, rows, :] = ls[k, tl + t, rows, :] + src[k, t]

    begin40 = l40 < 4
    zpad = jnp.zeros((42, 2, 8, 128), F32)
    for c in (ca, cb):
        c[:, :, pl.ds(0, 8), :] = zpad
        c[:, :, pl.ds(48, 8), :] = zpad

    def assemble(p, _):
        t = p // 16
        q = p - 16 * t
        shift = lax.rem(252 - 8 * q, 128)
        low = pltpu.roll(ls[0, t], shift, 1)
        high = pltpu.roll(ls[1, t], shift, 1)
        main = jnp.where(begin40, low, jnp.where(edge40, high, gs[p]))
        halo = jnp.where(begin40, high, jnp.where(edge40, low, zero40))
        g2[p, 0] = main
        g2[p, 1] = halo
        ca[p, 0, pl.ds(8, 40), :] = main * kc[0]
        ca[p, 1, pl.ds(8, 40), :] = halo * kc[1]
        return 0

    lax.fori_loop(0, 40, assemble, 0, unroll=UA)

    zc = jnp.zeros((2, 40, 128), F32)

    def clip(c):
        @pl.when(gx == 0)
        def _():
            for p in range(4):
                c[p, :, pl.ds(8, 40), :] = zc

        @pl.when(gx == nx - 1)
        def _():
            for p in range(36, 40):
                c[p, :, pl.ds(8, 40), :] = zc

    first40 = l40 == 0
    last40 = l40 == 127

    def coarse_sweep(c, v, lo, hi, unroll):
        def body(p, _):
            own = [c[p, h, pl.ds(8, 40), :] for h in range(2)]
            right = [pltpu.roll(own[h], 1, 1) for h in range(2)]
            left = [pltpu.roll(own[h], 127, 1) for h in range(2)]
            for h in range(2):
                total = c[p - 1, h, pl.ds(8, 40), :] + c[p + 1, h, pl.ds(8, 40), :]
                total = total + (c[p, h, pl.ds(7, 40), :] + c[p, h, pl.ds(9, 40), :])
                total = total + (own[h] + g2[p, h])
                total = total + jnp.where(first40, right[1 - h], right[h])
                total = total + jnp.where(last40, left[1 - h], left[h])
                v[p, h, pl.ds(8, 40), :] = total * kc[h]
            return 0

        lax.fori_loop(lo, hi, body, 0, unroll=unroll)
        clip(v)

    clip(ca)
    coarse_sweep(ca, cb, 1, 41, UC[0])
    coarse_sweep(cb, ca, 2, 38, UC[1])
    coarse_sweep(ca, cb, 3, 38, UC[2])

    def prolong_z(n, _):
        i = 11 * n
        block = [cb[pl.ds(3 + i, 11), h, pl.ds(8, 40), :].reshape(440, 128) for h in range(2)]
        got = dot3(jnp.concatenate(block, axis=1), wp[...])
        for h in range(2):
            fz[pl.ds(i, 11), h] = got[:, 128 * h : 128 * h + 128].reshape(11, 40, 128)
        return 0

    lax.fori_loop(0, 3, prolong_z, 0)

    sent(round0)
    sent(round1)
    for dx, dy, dz, copy in messages:
        pl.when(has_all(dx, dy, dz))(copy.wait_send)


def finish_kernel(u2, fz, out, ot, wt, out_sem):
    def prolong_y(j, slot):
        for h in range(2):
            here = fz[j, h, pl.ds(4, 32), :]
            wt[slot, h, pl.ds(0, 32, stride=2), :] = 0.5 * (fz[j, h, pl.ds(3, 32), :] + here)
            wt[slot, h, pl.ds(1, 32, stride=2), :] = here

    prolong_y(0, 0)

    def outgoing(x, n, h):
        return pltpu.make_async_copy(
            ot.at[pl.ds(x, n), h], out.at[pl.ds(x, n), :, pl.ds(128 * h, 128)], out_sem.at[h])

    def finish(i, _):
        slot = lax.rem(i + 1, 2)
        prolong_y(i + 1, slot)
        for h in range(2):
            here = wt[slot, h]
            mean = 0.5 * (wt[1 - slot, h] + here)
            ot[2 * i, h] = u2[2 * i + 3, h, pl.ds(8, 64), :] + mean
            ot[2 * i + 1, h] = u2[2 * i + 4, h, pl.ds(8, 64), :] + here
        for h in range(2):
            outgoing(2 * i, 2, h).start()
        return 0

    lax.fori_loop(0, 32, finish, 0, unroll=UF)
    for h in range(2):
        outgoing(0, 64, h).wait()


def on_device(start_field, right_side):
    v = pltpu.VMEM
    scratch = [
        v((66, 2, 80, 128), F32), v((66, 2, 80, 128), F32),
        v((69, 2, 64, 128), F32), v((2, 64, 128), F32), v((2, 2, 64, 128), F32),
        v((2, 4, 96, 128), F32), v((34, 40, 512), F32), v((512, 256), BF16), v((256, 256), BF16),
        v((40, 40, 128), F32), v((40, 40, 128), F32), v((2, 3, 40, 128), F32), v((2, 3, 40, 128), F32),
        v((3, 40, 128), F32), v((42, 2, 40, 128), F32), v((42, 2, 56, 128), F32), v((42, 2, 56, 128), F32),
    ]
    scratch += [v((SEND[dx][1], SEND[dy][1], 128), F32) for dx, dy in XY8]
    scratch += [v((2, TSEND[dx][1], SEND[dy][1], 128), F32) for dx, dy in XY8]
    scratch += [v((2, TSEND[dx][1], SEND[dy][1], 128), F32) for dx, dy in XY]
    dma = pltpu.SemaphoreType.DMA
    scratch += [dma((4,)), dma((2, 6)), dma((2, 6)), dma((8,)), dma((8,)), dma((8,)), dma((8,)),
                dma((9, 2)), dma((9, 2))]
    anywhere = pl.BlockSpec(memory_space=pltpu.HBM)
    vmem = pl.BlockSpec(memory_space=pltpu.VMEM)
    smoothed, correction = pl.pallas_call(
        kernel,
        out_shape=(v((71, 2, 80, 128), F32), v((33, 2, 40, 128), F32)),
        in_specs=[anywhere, anywhere],
        out_specs=(vmem, vmem),
        scratch_shapes=scratch,
        compiler_params=pltpu.CompilerParams(
            collective_id=0, has_side_effects=True, vmem_limit_bytes=54 * 1024 * 1024),
    )(start_field, right_side)
    return pl.pallas_call(
        finish_kernel,
        out_shape=jax.ShapeDtypeStruct(start_field.shape, F32),
        in_specs=[vmem, vmem],
        out_specs=anywhere,
        scratch_shapes=[v((64, 2, 64, 128), F32), v((2, 2, 64, 128), F32), dma((2,))],
        compiler_params=pltpu.CompilerParams(vmem_limit_bytes=12 * 1024 * 1024),
    )(smoothed, correction)


def solution(mesh):
    placed = P("gx", "gy", "gz")
    return jax.shard_map(on_device, mesh=mesh, in_specs=(placed, placed), out_specs=placed, check_vma=False)
```

```python
import functools

import jax
import jax.numpy as jnp
from jax import lax
from jax.experimental import pallas as pl
from jax.experimental.pallas import tpu as pltpu
from jax.sharding import PartitionSpec as P

MESH = pl.DeviceIdType.MESH
F32 = jnp.float32
BF16 = jnp.bfloat16
SEVENTH = 1.0 / 7.0
UE, UA, UF = 8, 8, 2
NI, GI, GO = 6, 4, 8
UC = (8, 6, 7)
AXES = ("gx", "gy", "gz")
SEND = {-1: (3, 4), 0: (3, 34), 1: (32, 5)}
LAND = {-1: 35, 0: 3, 1: 0}
TSEND = {-1: (0, 1), 0: (0, 3), 1: (2, 1)}
TLAND = {-1: 2, 0: 0, 1: 0}
XY = [(dx, dy) for dx in (-1, 0, 1) for dy in (-1, 0, 1)]
XY8 = [d for d in XY if d != (0, 0)]


def split3(v):
    hi = v.astype(BF16)
    rest = v - hi.astype(F32)
    mid = rest.astype(BF16)
    lo = (rest - mid.astype(F32)).astype(BF16)
    return hi, mid, lo


def dot3(v, weights):
    parts = [jnp.dot(p, weights, preferred_element_type=F32) for p in split3(v)]
    return (parts[2] + parts[1]) + parts[0]


def kernel(s_in, b_in, u2, fz, *scratch):
    (u0, u1, bv, ez, zr, at, qb, wr, wp, gm, gs, lh, ls, kc, g2, ca, cb, zs) = scratch[:18]
    rm = scratch[18:26]
    rl = scratch[26:34]
    rz = scratch[34:43]
    load_sem, f_send, f_recv, m_send, m_recv, l_send, l_recv, z_send, z_recv, h_send, h_recv = scratch[43:]

    gx, gy, gz = (lax.axis_index(a) for a in AXES)
    nx, ny, nz = (lax.axis_size(a) for a in AXES)
    me = {"gx": gx, "gy": gy, "gz": gz}
    size = {"gx": nx, "gy": ny, "gz": nz}

    def has(axis, d):
        if d == 0:
            return True
        return me[axis] < size[axis] - 1 if d > 0 else me[axis] > 0

    def has_all(dx, dy, dz):
        ok = None
        for axis, d in zip(AXES, (dx, dy, dz)):
            if d:
                here = has(axis, d)
                ok = here if ok is None else jnp.logical_and(ok, here)
        return ok

    def target(dx, dy, dz):
        return {a: me[a] + d for a, d in zip(AXES, (dx, dy, dz))}

    loads = []
    for h in range(2):
        lanes = pl.ds(128 * h, 128)
        loads.append(pltpu.make_async_copy(s_in.at[:, :, lanes], u0.at[pl.ds(1, 64), h, pl.ds(8, 64), :], load_sem.at[h]))
    for h in range(2):
        lanes = pl.ds(128 * h, 128)
        loads.append(pltpu.make_async_copy(b_in.at[:, :, lanes], bv.at[pl.ds(2, 64), h], load_sem.at[2 + h]))
    loads[0].start()
    loads[1].start()

    barrier = pltpu.get_barrier_semaphore()
    count = jnp.int32(0)
    for axis in AXES:
        for d in (-1, 1):
            ok = has(axis, d)
            count = count + ok.astype(jnp.int32)

            @pl.when(ok)
            def _():
                pl.semaphore_signal(barrier, inc=1, device_id={axis: me[axis] + d}, device_id_type=MESH)

    lane = lax.broadcasted_iota(jnp.int32, (64, 128), 1)
    first = lane == 0
    last = lane == 127
    group = lax.rem((lane + 1) // 2, 64)

    zplane = jnp.zeros((2, 80, 128), F32)
    zrow = jnp.zeros((1, 128), F32)

    @pl.when(gx == 0)
    def _():
        u0[0] = zplane
        u1[0] = zplane

    @pl.when(gx == nx - 1)
    def _():
        u0[65] = zplane
        u1[65] = zplane

    def zero_rows(row):
        def body(x, _):
            for h in range(2):
                u0[x, h, pl.ds(row, 1), :] = zrow
                u1[x, h, pl.ds(row, 1), :] = zrow
            return 0

        lax.fori_loop(1, 65, body, 0)

    @pl.when(gy == 0)
    def _():
        zero_rows(7)

    @pl.when(gy == ny - 1)
    def _():
        zero_rows(72)

    @pl.when(gz == 0)
    def _():
        zr[0, 0] = jnp.zeros((64, 128), F32)
        zr[1, 0] = jnp.zeros((64, 128), F32)

    @pl.when(gz == nz - 1)
    def _():
        zr[0, 1] = jnp.zeros((64, 128), F32)
        zr[1, 1] = jnp.zeros((64, 128), F32)

    for p in (0, 1, 2, 67, 68, 69, 70):
        u2[p] = zplane
    for p in (0, 1, 66, 67, 68):
        bv[p] = jnp.zeros((2, 64, 128), F32)
    at[...] = jnp.zeros(at.shape, F32)

    def coarse_of(column):
        inner = column - 128
        return jnp.where(column < 128, column, jnp.where(inner >= 64, inner - 128, inner + 128))

    zi = lax.broadcasted_iota(jnp.int32, (256, 256), 0)
    kci = coarse_of(lax.broadcasted_iota(jnp.int32, (256, 256), 1))
    d = zi - 2 * kci
    zero = jnp.zeros((256, 256), F32)
    plain = jnp.where(d == 1, -2.0, jnp.where((d == 0) | (d == 2), -1.0, zero))
    topz = (gz == nz - 1).astype(F32)
    edge = jnp.where((zi == 255) & (kci == 127), topz, zero)
    around = jnp.where((d >= 0) & (d <= 2), 2.0, jnp.where((d == -1) | (d == 3), 1.0, zero)) - edge
    wr[pl.ds(0, 256), :] = plain.astype(BF16)
    wr[pl.ds(256, 256), :] = around.astype(BF16)
    kr = coarse_of(lax.broadcasted_iota(jnp.int32, (256, 256), 0))
    d = lax.broadcasted_iota(jnp.int32, (256, 256), 1) - 2 * kr
    wp[...] = jnp.where(d == 1, 1.0, jnp.where((d == 0) | (d == 2), 0.5, zero)).astype(BF16)

    r40 = lax.broadcasted_iota(jnp.int32, (40, 128), 0)
    l40 = lax.broadcasted_iota(jnp.int32, (40, 128), 1)
    zero40 = jnp.zeros((40, 128), F32)
    low_y = jnp.where(gy > 0, 0, 4)
    high_y = jnp.where(gy < ny - 1, 40, 36)
    low_z = jnp.where(gz > 0, 124, 128)
    high_z = jnp.where(gz < nz - 1, 4, 0)
    rows_in = jnp.where((r40 >= low_y) & (r40 < high_y), SEVENTH, zero40)
    kc[0] = rows_in
    for p in (0, 1, 2, 37, 38, 39):
        gm[p] = zero40
        gs[p] = zero40
        g2[p, 1] = zero40
    kc[1] = jnp.where((l40 >= low_z) | (l40 < high_z), rows_in, zero40)
    topy = (gy == ny - 1).astype(F32)
    kc[2] = 0.5 - jnp.where(r40 == 35, 0.25 * topy, zero40)

    zpad = jnp.zeros((42, 2, 8, 128), F32)
    for c in (ca, cb):
        c[:, :, pl.ds(0, 8), :] = zpad
        c[:, :, pl.ds(48, 8), :] = zpad

    def faces(r, u):
        x_in = (slice(None), pl.ds(8, 64), slice(None))
        xs = pl.ds(1, 64)
        every = slice(None)
        plan = [
            ("gx", 1, u.at[(64,) + x_in], u.at[(0,) + x_in]),
            ("gx", -1, u.at[(1,) + x_in], u.at[(65,) + x_in]),
            ("gy", 1, u.at[xs, every, pl.ds(71, 1), every], u.at[xs, every, pl.ds(7, 1), every]),
            ("gy", -1, u.at[xs, every, pl.ds(8, 1), every], u.at[xs, every, pl.ds(72, 1), every]),
            ("gz", 1, ez.at[r], zr.at[r, 0]),
            ("gz", -1, ez.at[r], zr.at[r, 1]),
        ]
        done = []
        for k, (axis, dd, src, dst) in enumerate(plan):
            copy = pltpu.make_async_remote_copy(
                src_ref=src, dst_ref=dst, send_sem=f_send.at[r, k], recv_sem=f_recv.at[r, k],
                device_id={axis: me[axis] + dd}, device_id_type=MESH,
            )
            done.append((axis, dd, copy))
        return done

    def start(copies):
        for axis, dd, copy in copies:
            pl.when(has(axis, dd))(copy.start)

    def arrive(copies):
        for axis, dd, copy in copies:
            pl.when(has(axis, -dd))(copy.wait_recv)

    def sent(copies):
        for axis, dd, copy in copies:
            pl.when(has(axis, dd))(copy.wait_send)

    round0, round1 = faces(0, u0), faces(1, u1)

    loads[0].wait()
    loads[1].wait()
    loads[2].start()
    loads[3].start()
    pl.semaphore_wait(barrier, count)
    start(round0[:4])

    group8 = group[:8]
    first8, last8 = first[:8], last[:8]

    def pack(n, packed):
        for j in range(8):
            x = 8 * n + j
            both = jnp.where(first, u0[x + 1, 0, pl.ds(8, 64), :], u0[x + 1, 1, pl.ds(8, 64), :])
            packed = jnp.where(group == x, pltpu.roll(both, 2 * x, 1), packed)
        return packed

    ez[0] = lax.fori_loop(0, 8, pack, jnp.zeros((64, 128), F32))
    ez[1] = jnp.zeros((64, 128), F32)
    start(round0[4:])

    def beside_z(r, u, starts, x0, group_size):
        halo = [zr[r, 0, pl.ds(y, 8), :] for y in starts]
        for j in range(group_size):
            x = x0 + j
            shift = lax.rem(128 - 2 * x, 128)
            for k, y in enumerate(starts):
                side = pltpu.roll(halo[k], shift, 1)
                c = [u[x + 1, h, pl.ds(8 + y, 8), :] for h in range(2)]
                right = [pltpu.roll(c[h], 1, 1) for h in range(2)]
                left = [pltpu.roll(c[h], 127, 1) for h in range(2)]
                zs[j, k, 0] = jnp.where(first8, side, right[0]) + jnp.where(last8, left[1], left[0])
                zs[j, k, 1] = jnp.where(first8, right[0], right[1]) + jnp.where(last8, side, left[1])

    def pack_ends_of(v, starts, x0, group_size):
        packed = [ez[1, pl.ds(y, 8), :] for y in starts]
        for j in range(group_size):
            x = x0 + j
            here = group8 == x
            for k, y in enumerate(starts):
                both = jnp.where(first8, v[x + 1, 0, pl.ds(8 + y, 8), :], v[x + 1, 1, pl.ds(8 + y, 8), :])
                packed[k] = jnp.where(here, pltpu.roll(both, 2 * x, 1), packed[k])
        for k, y in enumerate(starts):
            ez[1, pl.ds(y, 8), :] = packed[k]

    def relax(u, v, off, starts, x0, group_size):
        def planes(p):
            return [[u[p, h, pl.ds(8 + y, 8), :] for h in range(2)] for y in starts]

        before, here = planes(x0), planes(x0 + 1)
        for j in range(group_size):
            x = x0 + j
            after = planes(x + 2)
            for k, y in enumerate(starts):
                for h in range(2):
                    total = (before[k][h] + after[k][h]) + (here[k][h] + bv[x + 2, h, pl.ds(y, 8), :])
                    total = total + (u[x + 1, h, pl.ds(7 + y, 8), :] + u[x + 1, h, pl.ds(9 + y, 8), :])
                    v[x + off, h, pl.ds(8 + y, 8), :] = (total + zs[j, k, h]) * SEVENTH
            before, here = here, after

    def pipelined(r, u, v, off, count, place, group_size):
        beside_z(r, u, *place(0), group_size)

        def body(n, _):
            if r == 0:
                pack_ends_of(v, *place(jnp.maximum(n - 1, 0)), group_size)
            relax(u, v, off, *place(n), group_size)
            beside_z(r, u, *place(jnp.minimum(n + 1, count - 1)), group_size)
            return 0

        lax.fori_loop(0, count, body, 0)
        if r == 0:
            pack_ends_of(v, *place(count - 1), group_size)

    def sweep(r, copies, u, v, off):
        arrive(copies[4:])
        even = lax.rem(lane, 2) == 0
        zr[r, 0] = jnp.where(even, pltpu.roll(zr[r, 0], 1, 1), pltpu.roll(zr[r, 1], 127, 1))
        arrive(copies[:2])
        every = 64 // GI

        def inner(n):
            y = 8 + 8 * NI * (n // every)
            return [pl.multiple_of(y + 8 * k, 8) for k in range(NI)], GI * lax.rem(n, every)

        pipelined(r, u, v, off, (6 // NI) * every, inner, GI)
        arrive(copies[2:4])
        pipelined(r, u, v, off, 64 // GO, lambda n: ([0, 56], GO * n), GO)

    loads[2].wait()
    loads[3].wait()
    sweep(0, round0, u0, u1, 1)
    start(round1)
    sweep(1, round1, u1, u2, 3)

    topx = gx == nx - 1

    def restrict(i, _):
        slot = lax.rem(i, 2)
        mid = jnp.where(jnp.logical_and(topx, i == 32), 2.75, 2.5).astype(F32)
        for h in range(2):
            w = [u2[2 * i + k, h, pl.ds(8, 64), :] for k in range(5)]
            b = [bv[2 * i + k, h] for k in range(3)]
            beside = w[1] + w[3]
            at[slot, h, pl.ds(16, 64), :] = 0.25 * beside + 0.5 * w[2]
            load = 0.25 * (b[0] + b[2]) + 0.5 * b[1]
            at[slot, 2 + h, pl.ds(16, 64), :] = (beside - 0.25 * (w[0] + w[4])) + (mid * w[2] - load)
        for h in range(2):
            a1 = [at[slot, h, pl.ds(8 + o, 40, stride=2), :] for o in (-1, 0, 1, 2, 3)]
            a2 = [at[slot, 2 + h, pl.ds(8 + o, 40, stride=2), :] for o in (0, 1, 2)]
            beside = a1[1] + a1[3]
            main = 0.25 * (a2[0] + a2[2]) + 0.5 * a2[1]
            main = main - (0.25 * (a1[0] + a1[4]) + 0.5 * beside) - kc[2] * a1[2]
            qb[i, :, pl.ds(128 * h, 128)] = main
            qb[i, :, pl.ds(256 + 128 * h, 128)] = 0.25 * beside + 0.5 * a1[2]
        return 0


    def restrict_half(n, _):
        i = 17 * n
        lax.fori_loop(i, i + 17, restrict, 0)
        got = dot3(qb[pl.ds(i, 17)].reshape(680, 512), wr[...])
        main = got[:, :128].reshape(17, 40, 128)
        gm[pl.ds(i + 3, 17)] = main
        gs[pl.ds(i + 3, 17)] = main
        g2[pl.ds(i + 3, 17), 1] = got[:, 128:].reshape(17, 40, 128)
        return 0

    def half_message(n, dy):
        ya, yn = SEND[dy]
        e = 0 if dy < 0 else 1
        return pltpu.make_async_remote_copy(
            src_ref=gm.at[pl.ds(3 + 17 * n, 17), pl.ds(ya, yn), :],
            dst_ref=rm[XY8.index((0, dy))].at[pl.ds(17 * n, 17)],
            send_sem=h_send.at[n, e], recv_sem=h_recv.at[n, e],
            device_id=target(0, dy, 0), device_id_type=MESH)

    mains = []
    for n, (dx, dy) in enumerate(XY8):
        if dx:
            (xa, xn), (ya, yn) = SEND[dx], SEND[dy]
            mains.append((dx, dy, n, pltpu.make_async_remote_copy(
                src_ref=gm.at[pl.ds(xa, xn), pl.ds(ya, yn), :], dst_ref=rm[n],
                send_sem=m_send.at[n], recv_sem=m_recv.at[n], device_id=target(dx, dy, 0), device_id_type=MESH)))
    mains.sort(key=lambda m: abs(m[1]))

    def half(n, _):
        restrict_half(n, 0)
        for dy in (-1, 1):
            pl.when(has("gy", dy))(lambda: half_message(n, dy).start())
        for dx, dy, _, copy in mains:
            ready = n == (0 if dx < 0 else 1)
            pl.when(jnp.logical_and(ready, has_all(dx, dy, 0)))(copy.start)
        return 0

    lax.fori_loop(0, 2, half, 0)

    edge40 = l40 >= 124
    oct40 = l40 // 8
    for t, (lo, hi) in enumerate(((0, 16), (16, 32), (32, 40))):

        def pack_ends(p, ends):
            main, halo = gm[p], g2[p, 1]
            q = p - 16 * t
            shift = lax.rem(8 * q + 4, 128)
            here = oct40 == q
            return (
                jnp.where(here, pltpu.roll(jnp.where(edge40, halo, main), shift, 1), ends[0]),
                jnp.where(here, pltpu.roll(jnp.where(edge40, main, halo), shift, 1), ends[1]),
            )

        ends = lax.fori_loop(lo, hi, pack_ends, (zero40, zero40), unroll=UE)
        for k in range(2):
            lh[k, t] = ends[k]
            ls[k, t] = ends[k]

    messages = []
    for n, (dx, dy) in enumerate(XY8):
        ya, yn = SEND[dy]
        ta, tn = TSEND[dx]
        messages.append((dx, dy, 0, n, pltpu.make_async_remote_copy(
            src_ref=lh.at[:, pl.ds(ta, tn), pl.ds(ya, yn), :], dst_ref=rl[n],
            send_sem=l_send.at[n], recv_sem=l_recv.at[n], device_id=target(dx, dy, 0), device_id_type=MESH)))
    for n, (dx, dy) in enumerate(XY):
        ya, yn = SEND[dy]
        ta, tn = TSEND[dx]
        for dz in (-1, 1):
            end = 1 if dz > 0 else 0
            messages.append((dx, dy, dz, n, pltpu.make_async_remote_copy(
                src_ref=lh.at[end, pl.ds(ta, tn), pl.ds(ya, yn), :], dst_ref=rz[n].at[1 - end],
                send_sem=z_send.at[n, end], recv_sem=z_recv.at[n, end],
                device_id=target(dx, dy, dz), device_id_type=MESH)))
    messages.sort(key=lambda m: (abs(m[0]) + abs(m[1]) + abs(m[2])))
    for dx, dy, dz, _, copy in messages:
        pl.when(has_all(dx, dy, dz))(copy.start)

    def add_main(dx, dy, n):
        xn, xl = SEND[dx][1], LAND[dx]
        rows = pl.ds(LAND[dy], SEND[dy][1])

        def add(p, _):
            gs[xl + p, rows, :] = gs[xl + p, rows, :] + rm[n][p]
            return 0

        lax.fori_loop(0, xn, add, 0, unroll=min(xn, 17))

    def take_half(dy):
        half_message(0, dy).wait_recv()
        half_message(1, dy).wait_recv()
        add_main(0, dy, XY8.index((0, dy)))

    def take_main(dx, dy, n, copy):
        copy.wait_recv()
        add_main(dx, dy, n)

    def take_ends(dx, dy, dz, n, copy):
        copy.wait_recv()
        rows, tl = pl.ds(LAND[dy], SEND[dy][1]), TLAND[dx]
        for k in (0, 1) if dz == 0 else (0,) if dz > 0 else (1,):
            src = rl[n] if dz == 0 else rz[n]
            for t in range(TSEND[dx][1]):
                ls[k, tl + t, rows, :] = ls[k, tl + t, rows, :] + src[k, t]

    for dy in (-1, 1):
        pl.when(has("gy", -dy))(functools.partial(take_half, dy))
    for dx, dy, n, copy in mains:
        pl.when(has_all(-dx, -dy, 0))(functools.partial(take_main, dx, dy, n, copy))
    for dx, dy, dz, n, copy in messages:
        pl.when(has_all(-dx, -dy, -dz))(functools.partial(take_ends, dx, dy, dz, n, copy))

    begin40 = l40 < 4
    def assemble(p, _):
        t = p // 16
        q = p - 16 * t
        shift = lax.rem(252 - 8 * q, 128)
        low = pltpu.roll(ls[0, t], shift, 1)
        high = pltpu.roll(ls[1, t], shift, 1)
        main = jnp.where(begin40, low, jnp.where(edge40, high, gs[p]))
        halo = jnp.where(begin40, high, jnp.where(edge40, low, zero40))
        g2[p, 0] = main
        g2[p, 1] = halo
        ca[p, 0, pl.ds(8, 40), :] = main * kc[0]
        ca[p, 1, pl.ds(8, 40), :] = halo * kc[1]
        return 0

    lax.fori_loop(0, 40, assemble, 0, unroll=UA)

    zc = jnp.zeros((2, 40, 128), F32)

    def clip(c):
        @pl.when(gx == 0)
        def _():
            for p in range(4):
                c[p, :, pl.ds(8, 40), :] = zc

        @pl.when(gx == nx - 1)
        def _():
            for p in range(36, 40):
                c[p, :, pl.ds(8, 40), :] = zc

    first40 = l40 == 0
    last40 = l40 == 127

    def coarse_sweep(c, v, lo, hi, many):
        def planes(p):
            return [c[p, h, pl.ds(8, 40), :] for h in range(2)]

        def body(n, _):
            p0 = lo + many * n
            before, own = planes(p0 - 1), planes(p0)
            for j in range(many):
                p = p0 + j
                after = planes(p + 1)
                right = [pltpu.roll(own[h], 1, 1) for h in range(2)]
                left = [pltpu.roll(own[h], 127, 1) for h in range(2)]
                for h in range(2):
                    total = (before[h] + after[h]) + (own[h] + g2[p, h])
                    total = total + (c[p, h, pl.ds(7, 40), :] + c[p, h, pl.ds(9, 40), :])
                    total = total + jnp.where(first40, right[1 - h], right[h])
                    total = total + jnp.where(last40, left[1 - h], left[h])
                    v[p, h, pl.ds(8, 40), :] = total * kc[h]
                before, own = own, after
            return 0

        lax.fori_loop(0, (hi - lo) // many, body, 0)
        clip(v)

    clip(ca)
    coarse_sweep(ca, cb, 1, 41, UC[0])
    coarse_sweep(cb, ca, 2, 38, UC[1])
    coarse_sweep(ca, cb, 3, 38, UC[2])

    def prolong_z(n, _):
        i = 11 * n
        block = [cb[pl.ds(3 + i, 11), h, pl.ds(8, 40), :].reshape(440, 128) for h in range(2)]
        got = dot3(jnp.concatenate(block, axis=1), wp[...])
        for h in range(2):
            fz[pl.ds(i, 11), h] = got[:, 128 * h : 128 * h + 128].reshape(11, 40, 128)
        return 0

    lax.fori_loop(0, 3, prolong_z, 0)

    sent(round0)
    sent(round1)
    for n in range(2):
        for dy in (-1, 1):
            pl.when(has("gy", dy))(half_message(n, dy).wait_send)
    for dx, dy, n, copy in mains:
        pl.when(has_all(dx, dy, 0))(copy.wait_send)
    for dx, dy, dz, n, copy in messages:
        pl.when(has_all(dx, dy, dz))(copy.wait_send)


def finish_kernel(u2, fz, out, ot, wt, out_sem):
    def prolong_y(j, slot):
        for h in range(2):
            here = fz[j, h, pl.ds(4, 32), :]
            wt[slot, h, pl.ds(0, 32, stride=2), :] = 0.5 * (fz[j, h, pl.ds(3, 32), :] + here)
            wt[slot, h, pl.ds(1, 32, stride=2), :] = here

    prolong_y(0, 0)

    def outgoing(x, n, h):
        return pltpu.make_async_copy(
            ot.at[pl.ds(x, n), h], out.at[pl.ds(x, n), :, pl.ds(128 * h, 128)], out_sem.at[h])

    def finish(i, _):
        slot = lax.rem(i + 1, 2)
        prolong_y(i + 1, slot)
        for h in range(2):
            here = wt[slot, h]
            mean = 0.5 * (wt[1 - slot, h] + here)
            ot[2 * i, h] = u2[2 * i + 3, h, pl.ds(8, 64), :] + mean
            ot[2 * i + 1, h] = u2[2 * i + 4, h, pl.ds(8, 64), :] + here
        for h in range(2):
            outgoing(2 * i, 2, h).start()
        return 0

    lax.fori_loop(0, 32, finish, 0, unroll=UF)
    for h in range(2):
        outgoing(0, 64, h).wait()


def on_device(start_field, right_side):
    v = pltpu.VMEM
    scratch = [
        v((66, 2, 80, 128), F32), v((66, 2, 80, 128), F32),
        v((69, 2, 64, 128), F32), v((2, 64, 128), F32), v((2, 2, 64, 128), F32),
        v((2, 4, 96, 128), F32), v((34, 40, 512), F32), v((512, 256), BF16), v((256, 256), BF16),
        v((40, 40, 128), F32), v((40, 40, 128), F32), v((2, 3, 40, 128), F32), v((2, 3, 40, 128), F32),
        v((3, 40, 128), F32), v((42, 2, 40, 128), F32), v((42, 2, 56, 128), F32), v((42, 2, 56, 128), F32),
        v((max(GI, GO), max(NI, 2), 2, 8, 128), F32),
    ]
    scratch += [v((SEND[dx][1], SEND[dy][1], 128), F32) for dx, dy in XY8]
    scratch += [v((2, TSEND[dx][1], SEND[dy][1], 128), F32) for dx, dy in XY8]
    scratch += [v((2, TSEND[dx][1], SEND[dy][1], 128), F32) for dx, dy in XY]
    dma = pltpu.SemaphoreType.DMA
    scratch += [dma((4,)), dma((2, 6)), dma((2, 6)), dma((8,)), dma((8,)), dma((8,)), dma((8,)),
                dma((9, 2)), dma((9, 2)), dma((2, 2)), dma((2, 2))]
    anywhere = pl.BlockSpec(memory_space=pltpu.HBM)
    vmem = pl.BlockSpec(memory_space=pltpu.VMEM)
    smoothed, correction = pl.pallas_call(
        kernel,
        out_shape=(v((71, 2, 80, 128), F32), v((33, 2, 40, 128), F32)),
        in_specs=[anywhere, anywhere],
        out_specs=(vmem, vmem),
        scratch_shapes=scratch,
        compiler_params=pltpu.CompilerParams(
            collective_id=0, has_side_effects=True, vmem_limit_bytes=54 * 1024 * 1024),
    )(start_field, right_side)
    return pl.pallas_call(
        finish_kernel,
        out_shape=jax.ShapeDtypeStruct(start_field.shape, F32),
        in_specs=[vmem, vmem],
        out_specs=anywhere,
        scratch_shapes=[v((64, 2, 64, 128), F32), v((2, 2, 64, 128), F32), dma((2,))],
        compiler_params=pltpu.CompilerParams(vmem_limit_bytes=12 * 1024 * 1024),
    )(smoothed, correction)


def solution(mesh):
    placed = P("gx", "gy", "gz")
    return jax.shard_map(on_device, mesh=mesh, in_specs=(placed, placed), out_specs=placed, check_vma=False)
```

```python
import functools

import jax
import jax.numpy as jnp
from jax import lax
from jax.experimental import pallas as pl
from jax.experimental.pallas import tpu as pltpu
from jax.sharding import PartitionSpec as P

MESH = pl.DeviceIdType.MESH
F32 = jnp.float32
BF16 = jnp.bfloat16
SEVENTH = 1.0 / 7.0
UE, UA, UF = 8, 8, 2
NI, GI, GH = 4, 8, 8
UC = (8, 6, 7)
AXES = ("gx", "gy", "gz")
SEND = {-1: (3, 4), 0: (3, 34), 1: (32, 5)}
LAND = {-1: 35, 0: 3, 1: 0}
TSEND = {-1: (0, 1), 0: (0, 3), 1: (2, 1)}
TLAND = {-1: 2, 0: 0, 1: 0}
XY = [(dx, dy) for dx in (-1, 0, 1) for dy in (-1, 0, 1)]
XY8 = [d for d in XY if d != (0, 0)]


def split3(v):
    hi = v.astype(BF16)
    rest = v - hi.astype(F32)
    mid = rest.astype(BF16)
    lo = (rest - mid.astype(F32)).astype(BF16)
    return hi, mid, lo


def dot3(v, weights):
    parts = [jnp.dot(p, weights, preferred_element_type=F32) for p in split3(v)]
    return (parts[2] + parts[1]) + parts[0]


def kernel(s_in, b_in, u2, fz, *scratch):
    (u0, u1, bv, ez, zr, at, qb, wr, wp, gm, gs, lh, ls, kc, g2, ca, cb, zs, hx, hy) = scratch[:20]
    rm = scratch[20:28]
    rl = scratch[28:36]
    rz = scratch[36:45]
    load_sem, f_send, f_recv, m_send, m_recv, l_send, l_recv, z_send, z_recv, h_send, h_recv = scratch[45:]

    gx, gy, gz = (lax.axis_index(a) for a in AXES)
    nx, ny, nz = (lax.axis_size(a) for a in AXES)
    me = {"gx": gx, "gy": gy, "gz": gz}
    size = {"gx": nx, "gy": ny, "gz": nz}

    def has(axis, d):
        if d == 0:
            return True
        return me[axis] < size[axis] - 1 if d > 0 else me[axis] > 0

    def has_all(dx, dy, dz):
        ok = None
        for axis, d in zip(AXES, (dx, dy, dz)):
            if d:
                here = has(axis, d)
                ok = here if ok is None else jnp.logical_and(ok, here)
        return ok

    def target(dx, dy, dz):
        return {a: me[a] + d for a, d in zip(AXES, (dx, dy, dz))}

    loads = []
    for h in range(2):
        lanes = pl.ds(128 * h, 128)
        loads.append(pltpu.make_async_copy(s_in.at[:, :, lanes], u0.at[pl.ds(1, 64), h, pl.ds(8, 64), :], load_sem.at[h]))
    for h in range(2):
        lanes = pl.ds(128 * h, 128)
        loads.append(pltpu.make_async_copy(b_in.at[:, :, lanes], bv.at[pl.ds(2, 64), h], load_sem.at[2 + h]))
    loads[0].start()
    loads[1].start()

    barrier = pltpu.get_barrier_semaphore()
    count = jnp.int32(0)
    for axis in AXES:
        for d in (-1, 1):
            ok = has(axis, d)
            count = count + ok.astype(jnp.int32)

            @pl.when(ok)
            def _():
                pl.semaphore_signal(barrier, inc=1, device_id={axis: me[axis] + d}, device_id_type=MESH)

    lane = lax.broadcasted_iota(jnp.int32, (64, 128), 1)
    first = lane == 0
    last = lane == 127
    group = lax.rem((lane + 1) // 2, 64)

    zplane = jnp.zeros((2, 80, 128), F32)
    zrow = jnp.zeros((1, 128), F32)
    for u in (u0, u1):
        u[0] = zplane
        u[65] = zplane

    def zero_rows(x, _):
        for h in range(2):
            for u in (u0, u1):
                u[x + 1, h, pl.ds(7, 1), :] = zrow
                u[x + 1, h, pl.ds(72, 1), :] = zrow
            for r in range(2):
                hy[r, 0, x, h, pl.ds(1, 7), :] = jnp.zeros((7, 128), F32)
                hy[r, 1, x, h, pl.ds(0, 7), :] = jnp.zeros((7, 128), F32)
        return 0

    lax.fori_loop(0, 64, zero_rows, 0, unroll=2)

    def zero_halo(side):
        def body(x, _):
            for r in range(2):
                for h in range(2):
                    hy[r, side, x, h, pl.ds(7 * side, 1), :] = zrow
            return 0

        lax.fori_loop(0, 64, body, 0)

    for side in range(2):
        d = 2 * side - 1

        @pl.when(jnp.logical_not(has("gy", d)))
        def _():
            zero_halo(side)

        @pl.when(jnp.logical_not(has("gz", d)))
        def _():
            for r in range(2):
                zr[r, side] = jnp.zeros((64, 128), F32)

    for p in (0, 1, 2, 67, 68, 69, 70):
        u2[p] = zplane
    for p in (0, 1, 66, 67, 68):
        bv[p] = jnp.zeros((2, 64, 128), F32)
    at[...] = jnp.zeros(at.shape, F32)

    def coarse_of(column):
        inner = column - 128
        return jnp.where(column < 128, column, jnp.where(inner >= 64, inner - 128, inner + 128))

    zi = lax.broadcasted_iota(jnp.int32, (256, 256), 0)
    kci = coarse_of(lax.broadcasted_iota(jnp.int32, (256, 256), 1))
    d = zi - 2 * kci
    zero = jnp.zeros((256, 256), F32)
    plain = jnp.where(d == 1, -2.0, jnp.where((d == 0) | (d == 2), -1.0, zero))
    topz = (gz == nz - 1).astype(F32)
    edge = jnp.where((zi == 255) & (kci == 127), topz, zero)
    around = jnp.where((d >= 0) & (d <= 2), 2.0, jnp.where((d == -1) | (d == 3), 1.0, zero)) - edge
    wr[pl.ds(0, 256), :] = plain.astype(BF16)
    wr[pl.ds(256, 256), :] = around.astype(BF16)
    kr = coarse_of(lax.broadcasted_iota(jnp.int32, (256, 256), 0))
    d = lax.broadcasted_iota(jnp.int32, (256, 256), 1) - 2 * kr
    wp[...] = jnp.where(d == 1, 1.0, jnp.where((d == 0) | (d == 2), 0.5, zero)).astype(BF16)

    r40 = lax.broadcasted_iota(jnp.int32, (40, 128), 0)
    l40 = lax.broadcasted_iota(jnp.int32, (40, 128), 1)
    zero40 = jnp.zeros((40, 128), F32)
    low_y = jnp.where(gy > 0, 0, 4)
    high_y = jnp.where(gy < ny - 1, 40, 36)
    low_z = jnp.where(gz > 0, 124, 128)
    high_z = jnp.where(gz < nz - 1, 4, 0)
    rows_in = jnp.where((r40 >= low_y) & (r40 < high_y), SEVENTH, zero40)
    kc[0] = rows_in
    for p in (0, 1, 2, 37, 38, 39):
        gm[p] = zero40
        gs[p] = zero40
        g2[p, 1] = zero40
    kc[1] = jnp.where((l40 >= low_z) | (l40 < high_z), rows_in, zero40)
    topy = (gy == ny - 1).astype(F32)
    kc[2] = 0.5 - jnp.where(r40 == 35, 0.25 * topy, zero40)

    zpad = jnp.zeros((42, 2, 8, 128), F32)
    for c in (ca, cb):
        c[:, :, pl.ds(0, 8), :] = zpad
        c[:, :, pl.ds(48, 8), :] = zpad

    def faces(r, u):
        x_in = (slice(None), pl.ds(8, 64), slice(None))
        xs = pl.ds(1, 64)
        every = slice(None)
        plan = [
            ("gx", 1, u.at[(64,) + x_in], hx.at[r, 0]),
            ("gx", -1, u.at[(1,) + x_in], hx.at[r, 1]),
            ("gy", 1, u.at[xs, every, pl.ds(71, 1), every], hy.at[r, 0, every, every, pl.ds(0, 1), every]),
            ("gy", -1, u.at[xs, every, pl.ds(8, 1), every], hy.at[r, 1, every, every, pl.ds(7, 1), every]),
            ("gz", 1, ez.at[r], zr.at[r, 0]),
            ("gz", -1, ez.at[r], zr.at[r, 1]),
        ]
        done = []
        for k, (axis, dd, src, dst) in enumerate(plan):
            copy = pltpu.make_async_remote_copy(
                src_ref=src, dst_ref=dst, send_sem=f_send.at[r, k], recv_sem=f_recv.at[r, k],
                device_id={axis: me[axis] + dd}, device_id_type=MESH,
            )
            done.append((axis, dd, copy))
        return done

    def start(copies):
        for axis, dd, copy in copies:
            pl.when(has(axis, dd))(copy.start)

    def arrive(copies):
        for axis, dd, copy in copies:
            pl.when(has(axis, -dd))(copy.wait_recv)

    def sent(copies):
        for axis, dd, copy in copies:
            pl.when(has(axis, dd))(copy.wait_send)

    round0, round1 = faces(0, u0), faces(1, u1)

    loads[0].wait()
    loads[1].wait()
    loads[2].start()
    loads[3].start()
    pl.semaphore_wait(barrier, count)
    start(round0[:4])

    first8, last8 = first[:8], last[:8]

    def pack_faces(r, u):
        def pack(n, packed):
            for j in range(8):
                x = 8 * n + j
                both = jnp.where(first, u[x + 1, 0, pl.ds(8, 64), :], u[x + 1, 1, pl.ds(8, 64), :])
                packed = jnp.where(group == x, pltpu.roll(both, 2 * x, 1), packed)
            return packed

        ez[r] = lax.fori_loop(0, 8, pack, jnp.zeros((64, 128), F32))

    pack_faces(0, u0)
    start(round0[4:])
    first8, last8 = first[:8], last[:8]
    zero8 = jnp.zeros((8, 128), F32)

    def beside_z(u, starts, x0, group_size):
        for j in range(group_size):
            for k, y in enumerate(starts):
                c = [u[x0 + j + 1, h, pl.ds(8 + y, 8), :] for h in range(2)]
                right = [pltpu.roll(c[h], 1, 1) for h in range(2)]
                left = [pltpu.roll(c[h], 127, 1) for h in range(2)]
                zs[j, k, 0] = jnp.where(first8, zero8, right[0]) + jnp.where(last8, left[1], left[0])
                zs[j, k, 1] = jnp.where(first8, right[0], right[1]) + jnp.where(last8, zero8, left[1])

    def relax(u, v, off, starts, x0, group_size):
        def planes(p):
            return [[u[p, h, pl.ds(8 + y, 8), :] for h in range(2)] for y in starts]

        before, here = planes(x0), planes(x0 + 1)
        for j in range(group_size):
            x = x0 + j
            after = planes(x + 2)
            for k, y in enumerate(starts):
                for h in range(2):
                    total = (before[k][h] + after[k][h]) + (here[k][h] + bv[x + 2, h, pl.ds(y, 8), :])
                    total = total + (u[x + 1, h, pl.ds(7 + y, 8), :] + u[x + 1, h, pl.ds(9 + y, 8), :])
                    v[x + off, h, pl.ds(8 + y, 8), :] = (total + zs[j, k, h]) * SEVENTH
            before, here = here, after

    def sweep(u, v, off):
        every = 64 // GI
        count = (8 // NI) * every

        def place(n):
            y = 8 * NI * (n // every)
            return [pl.multiple_of(y + 8 * k, 8) for k in range(NI)], GI * lax.rem(n, every)

        beside_z(u, *place(0), GI)

        def body(n, _):
            relax(u, v, off, *place(n), GI)
            beside_z(u, *place(jnp.minimum(n + 1, count - 1)), GI)
            return 0

        lax.fori_loop(0, count, body, 0)

    def add_halos(r, copies, v, off):
        arrive(copies)
        even = lax.rem(lane, 2) == 0
        zr[r, 0] = jnp.where(even, pltpu.roll(zr[r, 0], 1, 1), pltpu.roll(zr[r, 1], 127, 1)) * SEVENTH
        for side, p in enumerate((off, off + 63)):

            @pl.when(has("gx", 2 * side - 1))
            def _():
                for h in range(2):
                    v[p, h, pl.ds(8, 64), :] = v[p, h, pl.ds(8, 64), :] + hx[r, side, h] * SEVENTH

        def body(n, _):
            for j in range(GH):
                x = GH * n + j
                side = pltpu.roll(zr[r, 0], lax.rem(128 - 2 * x, 128), 1)
                for h in range(2):
                    for k in range(8):
                        at_end = jnp.where(last8 if h else first8, side[8 * k : 8 * k + 8], zero8)
                        if k in (0, 7):
                            at_end = at_end + hy[r, k // 7, x, h] * SEVENTH
                        rows = pl.ds(8 + 8 * k, 8)
                        v[x + off, h, rows, :] = v[x + off, h, rows, :] + at_end
            return 0

        lax.fori_loop(0, 64 // GH, body, 0)

    loads[2].wait()
    loads[3].wait()
    sweep(u0, u1, 1)
    add_halos(0, round0, u1, 1)
    start(round1[:4])
    pack_faces(1, u1)
    start(round1[4:])
    sweep(u1, u2, 3)
    add_halos(1, round1, u2, 3)

    topx = gx == nx - 1

    def restrict(i, _):
        slot = lax.rem(i, 2)
        mid = jnp.where(jnp.logical_and(topx, i == 32), 2.75, 2.5).astype(F32)
        for h in range(2):
            w = [u2[2 * i + k, h, pl.ds(8, 64), :] for k in range(5)]
            b = [bv[2 * i + k, h] for k in range(3)]
            beside = w[1] + w[3]
            at[slot, h, pl.ds(16, 64), :] = 0.25 * beside + 0.5 * w[2]
            load = 0.25 * (b[0] + b[2]) + 0.5 * b[1]
            at[slot, 2 + h, pl.ds(16, 64), :] = (beside - 0.25 * (w[0] + w[4])) + (mid * w[2] - load)
        for h in range(2):
            a1 = [at[slot, h, pl.ds(8 + o, 40, stride=2), :] for o in (-1, 0, 1, 2, 3)]
            a2 = [at[slot, 2 + h, pl.ds(8 + o, 40, stride=2), :] for o in (0, 1, 2)]
            beside = a1[1] + a1[3]
            main = 0.25 * (a2[0] + a2[2]) + 0.5 * a2[1]
            main = main - (0.25 * (a1[0] + a1[4]) + 0.5 * beside) - kc[2] * a1[2]
            qb[i, :, pl.ds(128 * h, 128)] = main
            qb[i, :, pl.ds(256 + 128 * h, 128)] = 0.25 * beside + 0.5 * a1[2]
        return 0


    def restrict_half(n, _):
        i = 17 * n
        lax.fori_loop(i, i + 17, restrict, 0)
        got = dot3(qb[pl.ds(i, 17)].reshape(680, 512), wr[...])
        main = got[:, :128].reshape(17, 40, 128)
        gm[pl.ds(i + 3, 17)] = main
        gs[pl.ds(i + 3, 17)] = main
        g2[pl.ds(i + 3, 17), 1] = got[:, 128:].reshape(17, 40, 128)
        return 0

    def half_message(n, dy):
        ya, yn = SEND[dy]
        e = 0 if dy < 0 else 1
        return pltpu.make_async_remote_copy(
            src_ref=gm.at[pl.ds(3 + 17 * n, 17), pl.ds(ya, yn), :],
            dst_ref=rm[XY8.index((0, dy))].at[pl.ds(17 * n, 17)],
            send_sem=h_send.at[n, e], recv_sem=h_recv.at[n, e],
            device_id=target(0, dy, 0), device_id_type=MESH)

    mains = []
    for n, (dx, dy) in enumerate(XY8):
        if dx:
            (xa, xn), (ya, yn) = SEND[dx], SEND[dy]
            mains.append((dx, dy, n, pltpu.make_async_remote_copy(
                src_ref=gm.at[pl.ds(xa, xn), pl.ds(ya, yn), :], dst_ref=rm[n],
                send_sem=m_send.at[n], recv_sem=m_recv.at[n], device_id=target(dx, dy, 0), device_id_type=MESH)))
    mains.sort(key=lambda m: abs(m[1]))

    def half(n, _):
        restrict_half(n, 0)
        for dy in (-1, 1):
            pl.when(has("gy", dy))(lambda: half_message(n, dy).start())
        for dx, dy, _, copy in mains:
            ready = n == (0 if dx < 0 else 1)
            pl.when(jnp.logical_and(ready, has_all(dx, dy, 0)))(copy.start)
        return 0

    lax.fori_loop(0, 2, half, 0)

    edge40 = l40 >= 124
    oct40 = l40 // 8
    for t, (lo, hi) in enumerate(((0, 16), (16, 32), (32, 40))):

        def pack_ends(p, ends):
            main, halo = gm[p], g2[p, 1]
            q = p - 16 * t
            shift = lax.rem(8 * q + 4, 128)
            here = oct40 == q
            return (
                jnp.where(here, pltpu.roll(jnp.where(edge40, halo, main), shift, 1), ends[0]),
                jnp.where(here, pltpu.roll(jnp.where(edge40, main, halo), shift, 1), ends[1]),
            )

        ends = lax.fori_loop(lo, hi, pack_ends, (zero40, zero40), unroll=UE)
        for k in range(2):
            lh[k, t] = ends[k]
            ls[k, t] = ends[k]

    messages = []
    for n, (dx, dy) in enumerate(XY8):
        ya, yn = SEND[dy]
        ta, tn = TSEND[dx]
        messages.append((dx, dy, 0, n, pltpu.make_async_remote_copy(
            src_ref=lh.at[:, pl.ds(ta, tn), pl.ds(ya, yn), :], dst_ref=rl[n],
            send_sem=l_send.at[n], recv_sem=l_recv.at[n], device_id=target(dx, dy, 0), device_id_type=MESH)))
    for n, (dx, dy) in enumerate(XY):
        ya, yn = SEND[dy]
        ta, tn = TSEND[dx]
        for dz in (-1, 1):
            end = 1 if dz > 0 else 0
            messages.append((dx, dy, dz, n, pltpu.make_async_remote_copy(
                src_ref=lh.at[end, pl.ds(ta, tn), pl.ds(ya, yn), :], dst_ref=rz[n].at[1 - end],
                send_sem=z_send.at[n, end], recv_sem=z_recv.at[n, end],
                device_id=target(dx, dy, dz), device_id_type=MESH)))
    messages.sort(key=lambda m: (abs(m[0]) + abs(m[1]) + abs(m[2])))
    for dx, dy, dz, _, copy in messages:
        pl.when(has_all(dx, dy, dz))(copy.start)

    def add_main(dx, dy, n):
        xn, xl = SEND[dx][1], LAND[dx]
        rows = pl.ds(LAND[dy], SEND[dy][1])

        def add(p, _):
            gs[xl + p, rows, :] = gs[xl + p, rows, :] + rm[n][p]
            return 0

        lax.fori_loop(0, xn, add, 0, unroll=min(xn, 17))

    def take_half(dy):
        half_message(0, dy).wait_recv()
        half_message(1, dy).wait_recv()
        add_main(0, dy, XY8.index((0, dy)))

    def take_main(dx, dy, n, copy):
        copy.wait_recv()
        add_main(dx, dy, n)

    def take_ends(dx, dy, dz, n, copy):
        copy.wait_recv()
        rows, tl = pl.ds(LAND[dy], SEND[dy][1]), TLAND[dx]
        for k in (0, 1) if dz == 0 else (0,) if dz > 0 else (1,):
            src = rl[n] if dz == 0 else rz[n]
            for t in range(TSEND[dx][1]):
                ls[k, tl + t, rows, :] = ls[k, tl + t, rows, :] + src[k, t]

    for dy in (-1, 1):
        pl.when(has("gy", -dy))(functools.partial(take_half, dy))
    for dx, dy, n, copy in mains:
        pl.when(has_all(-dx, -dy, 0))(functools.partial(take_main, dx, dy, n, copy))
    for dx, dy, dz, n, copy in messages:
        pl.when(has_all(-dx, -dy, -dz))(functools.partial(take_ends, dx, dy, dz, n, copy))

    begin40 = l40 < 4
    def assemble(p, _):
        t = p // 16
        q = p - 16 * t
        shift = lax.rem(252 - 8 * q, 128)
        low = pltpu.roll(ls[0, t], shift, 1)
        high = pltpu.roll(ls[1, t], shift, 1)
        main = jnp.where(begin40, low, jnp.where(edge40, high, gs[p]))
        halo = jnp.where(begin40, high, jnp.where(edge40, low, zero40))
        g2[p, 0] = main
        g2[p, 1] = halo
        ca[p, 0, pl.ds(8, 40), :] = main * kc[0]
        ca[p, 1, pl.ds(8, 40), :] = halo * kc[1]
        return 0

    lax.fori_loop(0, 40, assemble, 0, unroll=UA)

    zc = jnp.zeros((2, 40, 128), F32)

    def clip(c):
        @pl.when(gx == 0)
        def _():
            for p in range(4):
                c[p, :, pl.ds(8, 40), :] = zc

        @pl.when(gx == nx - 1)
        def _():
            for p in range(36, 40):
                c[p, :, pl.ds(8, 40), :] = zc

    first40 = l40 == 0
    last40 = l40 == 127

    def coarse_sweep(c, v, lo, hi, many):
        def planes(p):
            return [c[p, h, pl.ds(8, 40), :] for h in range(2)]

        def body(n, _):
            p0 = lo + many * n
            before, own = planes(p0 - 1), planes(p0)
            for j in range(many):
                p = p0 + j
                after = planes(p + 1)
                right = [pltpu.roll(own[h], 1, 1) for h in range(2)]
                left = [pltpu.roll(own[h], 127, 1) for h in range(2)]
                for h in range(2):
                    total = (before[h] + after[h]) + (own[h] + g2[p, h])
                    total = total + (c[p, h, pl.ds(7, 40), :] + c[p, h, pl.ds(9, 40), :])
                    total = total + jnp.where(first40, right[1 - h], right[h])
                    total = total + jnp.where(last40, left[1 - h], left[h])
                    v[p, h, pl.ds(8, 40), :] = total * kc[h]
                before, own = own, after
            return 0

        lax.fori_loop(0, (hi - lo) // many, body, 0)
        clip(v)

    clip(ca)
    coarse_sweep(ca, cb, 1, 41, UC[0])
    coarse_sweep(cb, ca, 2, 38, UC[1])
    coarse_sweep(ca, cb, 3, 38, UC[2])

    def prolong_z(n, _):
        i = 11 * n
        block = [cb[pl.ds(3 + i, 11), h, pl.ds(8, 40), :].reshape(440, 128) for h in range(2)]
        got = dot3(jnp.concatenate(block, axis=1), wp[...])
        for h in range(2):
            fz[pl.ds(i, 11), h] = got[:, 128 * h : 128 * h + 128].reshape(11, 40, 128)
        return 0

    lax.fori_loop(0, 3, prolong_z, 0)

    sent(round0)
    sent(round1)
    for n in range(2):
        for dy in (-1, 1):
            pl.when(has("gy", dy))(half_message(n, dy).wait_send)
    for dx, dy, n, copy in mains:
        pl.when(has_all(dx, dy, 0))(copy.wait_send)
    for dx, dy, dz, n, copy in messages:
        pl.when(has_all(dx, dy, dz))(copy.wait_send)


def finish_kernel(u2, fz, out, ot, wt, out_sem):
    def prolong_y(j, slot):
        for h in range(2):
            here = fz[j, h, pl.ds(4, 32), :]
            wt[slot, h, pl.ds(0, 32, stride=2), :] = 0.5 * (fz[j, h, pl.ds(3, 32), :] + here)
            wt[slot, h, pl.ds(1, 32, stride=2), :] = here

    prolong_y(0, 0)

    def outgoing(x, n, h):
        return pltpu.make_async_copy(
            ot.at[pl.ds(x, n), h], out.at[pl.ds(x, n), :, pl.ds(128 * h, 128)], out_sem.at[h])

    def finish(i, _):
        slot = lax.rem(i + 1, 2)
        prolong_y(i + 1, slot)
        for h in range(2):
            here = wt[slot, h]
            mean = 0.5 * (wt[1 - slot, h] + here)
            ot[2 * i, h] = u2[2 * i + 3, h, pl.ds(8, 64), :] + mean
            ot[2 * i + 1, h] = u2[2 * i + 4, h, pl.ds(8, 64), :] + here
        for h in range(2):
            outgoing(2 * i, 2, h).start()
        return 0

    lax.fori_loop(0, 32, finish, 0, unroll=UF)
    for h in range(2):
        outgoing(0, 64, h).wait()


def on_device(start_field, right_side):
    v = pltpu.VMEM
    scratch = [
        v((66, 2, 80, 128), F32), v((66, 2, 80, 128), F32),
        v((69, 2, 64, 128), F32), v((2, 64, 128), F32), v((2, 2, 64, 128), F32),
        v((2, 4, 96, 128), F32), v((34, 40, 512), F32), v((512, 256), BF16), v((256, 256), BF16),
        v((40, 40, 128), F32), v((40, 40, 128), F32), v((2, 3, 40, 128), F32), v((2, 3, 40, 128), F32),
        v((3, 40, 128), F32), v((42, 2, 40, 128), F32), v((42, 2, 56, 128), F32), v((42, 2, 56, 128), F32),
        v((GI, NI, 2, 8, 128), F32),
        v((2, 2, 2, 64, 128), F32), v((2, 2, 64, 2, 8, 128), F32),
    ]
    scratch += [v((SEND[dx][1], SEND[dy][1], 128), F32) for dx, dy in XY8]
    scratch += [v((2, TSEND[dx][1], SEND[dy][1], 128), F32) for dx, dy in XY8]
    scratch += [v((2, TSEND[dx][1], SEND[dy][1], 128), F32) for dx, dy in XY]
    dma = pltpu.SemaphoreType.DMA
    scratch += [dma((4,)), dma((2, 6)), dma((2, 6)), dma((8,)), dma((8,)), dma((8,)), dma((8,)),
                dma((9, 2)), dma((9, 2)), dma((2, 2)), dma((2, 2))]
    anywhere = pl.BlockSpec(memory_space=pltpu.HBM)
    vmem = pl.BlockSpec(memory_space=pltpu.VMEM)
    smoothed, correction = pl.pallas_call(
        kernel,
        out_shape=(v((71, 2, 80, 128), F32), v((33, 2, 40, 128), F32)),
        in_specs=[anywhere, anywhere],
        out_specs=(vmem, vmem),
        scratch_shapes=scratch,
        compiler_params=pltpu.CompilerParams(
            collective_id=0, has_side_effects=True, vmem_limit_bytes=54 * 1024 * 1024),
    )(start_field, right_side)
    return pl.pallas_call(
        finish_kernel,
        out_shape=jax.ShapeDtypeStruct(start_field.shape, F32),
        in_specs=[vmem, vmem],
        out_specs=anywhere,
        scratch_shapes=[v((64, 2, 64, 128), F32), v((2, 2, 64, 128), F32), dma((2,))],
        compiler_params=pltpu.CompilerParams(vmem_limit_bytes=12 * 1024 * 1024),
    )(smoothed, correction)


def solution(mesh):
    placed = P("gx", "gy", "gz")
    return jax.shard_map(on_device, mesh=mesh, in_specs=(placed, placed), out_specs=placed, check_vma=False)
```

```python
import functools

import jax
import jax.numpy as jnp
from jax import lax
from jax.experimental import pallas as pl
from jax.experimental.pallas import tpu as pltpu
from jax.sharding import PartitionSpec as P

MESH = pl.DeviceIdType.MESH
F32 = jnp.float32
BF16 = jnp.bfloat16
SEVENTH = 1.0 / 7.0
UE, UA, UF = 8, 8, 2
NI, GI, GH = 4, 8, 32
UC = (8, 6, 7)
AXES = ("gx", "gy", "gz")
SEND = {-1: (3, 4), 0: (3, 34), 1: (32, 5)}
LAND = {-1: 35, 0: 3, 1: 0}
TSEND = {-1: (0, 1), 0: (0, 3), 1: (2, 1)}
TLAND = {-1: 2, 0: 0, 1: 0}
XY = [(dx, dy) for dx in (-1, 0, 1) for dy in (-1, 0, 1)]
XY8 = [d for d in XY if d != (0, 0)]


def split3(v):
    hi = v.astype(BF16)
    rest = v - hi.astype(F32)
    mid = rest.astype(BF16)
    lo = (rest - mid.astype(F32)).astype(BF16)
    return hi, mid, lo


def dot3(v, weights):
    parts = [jnp.dot(p, weights, preferred_element_type=F32) for p in split3(v)]
    return (parts[2] + parts[1]) + parts[0]


def kernel(s_in, b_in, u2, fz, *scratch):
    (u0, u1, bv, ez, zr, at, qb, wr, wp, gm, gs, lh, ls, kc, g2, ca, cb, zs, hx, hy) = scratch[:20]
    rm = scratch[20:28]
    rl = scratch[28:36]
    rz = scratch[36:45]
    load_sem, f_send, f_recv, m_send, m_recv, l_send, l_recv, z_send, z_recv, h_send, h_recv = scratch[45:]

    gx, gy, gz = (lax.axis_index(a) for a in AXES)
    nx, ny, nz = (lax.axis_size(a) for a in AXES)
    me = {"gx": gx, "gy": gy, "gz": gz}
    size = {"gx": nx, "gy": ny, "gz": nz}

    def has(axis, d):
        if d == 0:
            return True
        return me[axis] < size[axis] - 1 if d > 0 else me[axis] > 0

    def has_all(dx, dy, dz):
        ok = None
        for axis, d in zip(AXES, (dx, dy, dz)):
            if d:
                here = has(axis, d)
                ok = here if ok is None else jnp.logical_and(ok, here)
        return ok

    def target(dx, dy, dz):
        return {a: me[a] + d for a, d in zip(AXES, (dx, dy, dz))}

    loads = []
    for h in range(2):
        lanes = pl.ds(128 * h, 128)
        loads.append(pltpu.make_async_copy(s_in.at[:, :, lanes], u0.at[pl.ds(1, 64), h, pl.ds(8, 64), :], load_sem.at[h]))
    for h in range(2):
        lanes = pl.ds(128 * h, 128)
        loads.append(pltpu.make_async_copy(b_in.at[:, :, lanes], bv.at[pl.ds(2, 64), h], load_sem.at[2 + h]))
    loads[0].start()
    loads[1].start()

    barrier = pltpu.get_barrier_semaphore()
    count = jnp.int32(0)
    for axis in AXES:
        for d in (-1, 1):
            ok = has(axis, d)
            count = count + ok.astype(jnp.int32)

            @pl.when(ok)
            def _():
                pl.semaphore_signal(barrier, inc=1, device_id={axis: me[axis] + d}, device_id_type=MESH)

    lane = lax.broadcasted_iota(jnp.int32, (64, 128), 1)
    first = lane == 0
    last = lane == 127
    group = lax.rem((lane + 1) // 2, 64)

    zplane = jnp.zeros((2, 80, 128), F32)
    zrow = jnp.zeros((1, 128), F32)
    for u in (u0, u1):
        u[0] = zplane
        u[65] = zplane

    def zero_rows(x, _):
        for h in range(2):
            for u in (u0, u1):
                u[x + 1, h, pl.ds(7, 1), :] = zrow
                u[x + 1, h, pl.ds(72, 1), :] = zrow
            for r in range(2):
                hy[r, 0, x, h, pl.ds(1, 7), :] = jnp.zeros((7, 128), F32)
                hy[r, 1, x, h, pl.ds(0, 7), :] = jnp.zeros((7, 128), F32)
        return 0

    lax.fori_loop(0, 64, zero_rows, 0, unroll=2)

    def zero_halo(side):
        def body(x, _):
            for r in range(2):
                for h in range(2):
                    hy[r, side, x, h, pl.ds(7 * side, 1), :] = zrow
            return 0

        lax.fori_loop(0, 64, body, 0)

    for side in range(2):
        d = 2 * side - 1

        @pl.when(jnp.logical_not(has("gy", d)))
        def _():
            zero_halo(side)

        @pl.when(jnp.logical_not(has("gz", d)))
        def _():
            for r in range(2):
                zr[r, side] = jnp.zeros((64, 128), F32)

    for p in (0, 1, 2, 67, 68, 69, 70):
        u2[p] = zplane
    for p in (0, 1, 66, 67, 68):
        bv[p] = jnp.zeros((2, 64, 128), F32)
    at[...] = jnp.zeros(at.shape, F32)

    def coarse_of(column):
        inner = column - 128
        return jnp.where(column < 128, column, jnp.where(inner >= 64, inner - 128, inner + 128))

    zi = lax.broadcasted_iota(jnp.int32, (256, 256), 0)
    kci = coarse_of(lax.broadcasted_iota(jnp.int32, (256, 256), 1))
    d = zi - 2 * kci
    zero = jnp.zeros((256, 256), F32)
    plain = jnp.where(d == 1, -2.0, jnp.where((d == 0) | (d == 2), -1.0, zero))
    topz = (gz == nz - 1).astype(F32)
    edge = jnp.where((zi == 255) & (kci == 127), topz, zero)
    around = jnp.where((d >= 0) & (d <= 2), 2.0, jnp.where((d == -1) | (d == 3), 1.0, zero)) - edge
    wr[pl.ds(0, 256), :] = plain.astype(BF16)
    wr[pl.ds(256, 256), :] = around.astype(BF16)
    kr = coarse_of(lax.broadcasted_iota(jnp.int32, (256, 256), 0))
    d = lax.broadcasted_iota(jnp.int32, (256, 256), 1) - 2 * kr
    wp[...] = jnp.where(d == 1, 1.0, jnp.where((d == 0) | (d == 2), 0.5, zero)).astype(BF16)

    r40 = lax.broadcasted_iota(jnp.int32, (40, 128), 0)
    l40 = lax.broadcasted_iota(jnp.int32, (40, 128), 1)
    zero40 = jnp.zeros((40, 128), F32)
    low_y = jnp.where(gy > 0, 0, 4)
    high_y = jnp.where(gy < ny - 1, 40, 36)
    low_z = jnp.where(gz > 0, 124, 128)
    high_z = jnp.where(gz < nz - 1, 4, 0)
    rows_in = jnp.where((r40 >= low_y) & (r40 < high_y), SEVENTH, zero40)
    kc[0] = rows_in
    for p in (0, 1, 2, 37, 38, 39):
        gm[p] = zero40
        gs[p] = zero40
        g2[p, 1] = zero40
    kc[1] = jnp.where((l40 >= low_z) | (l40 < high_z), rows_in, zero40)
    topy = (gy == ny - 1).astype(F32)
    kc[2] = 0.5 - jnp.where(r40 == 35, 0.25 * topy, zero40)

    zpad = jnp.zeros((42, 2, 8, 128), F32)
    for c in (ca, cb):
        c[:, :, pl.ds(0, 8), :] = zpad
        c[:, :, pl.ds(48, 8), :] = zpad

    def faces(r, u):
        x_in = (slice(None), pl.ds(8, 64), slice(None))
        xs = pl.ds(1, 64)
        every = slice(None)
        plan = [
            ("gx", 1, u.at[(64,) + x_in], hx.at[r, 0]),
            ("gx", -1, u.at[(1,) + x_in], hx.at[r, 1]),
            ("gy", 1, u.at[xs, every, pl.ds(71, 1), every], hy.at[r, 0, every, every, pl.ds(0, 1), every]),
            ("gy", -1, u.at[xs, every, pl.ds(8, 1), every], hy.at[r, 1, every, every, pl.ds(7, 1), every]),
            ("gz", 1, ez.at[r], zr.at[r, 0]),
            ("gz", -1, ez.at[r], zr.at[r, 1]),
        ]
        done = []
        for k, (axis, dd, src, dst) in enumerate(plan):
            copy = pltpu.make_async_remote_copy(
                src_ref=src, dst_ref=dst, send_sem=f_send.at[r, k], recv_sem=f_recv.at[r, k],
                device_id={axis: me[axis] + dd}, device_id_type=MESH,
            )
            done.append((axis, dd, copy))
        return done

    def start(copies):
        for axis, dd, copy in copies:
            pl.when(has(axis, dd))(copy.start)

    def arrive(copies):
        for axis, dd, copy in copies:
            pl.when(has(axis, -dd))(copy.wait_recv)

    def sent(copies):
        for axis, dd, copy in copies:
            pl.when(has(axis, dd))(copy.wait_send)

    round0, round1 = faces(0, u0), faces(1, u1)

    loads[0].wait()
    loads[1].wait()
    loads[2].start()
    loads[3].start()
    pl.semaphore_wait(barrier, count)
    start(round0[:4])

    first8, last8 = first[:8], last[:8]

    def pack_faces(r, u):
        def pack(n, packed):
            for j in range(8):
                x = 8 * n + j
                both = jnp.where(first, u[x + 1, 0, pl.ds(8, 64), :], u[x + 1, 1, pl.ds(8, 64), :])
                packed = jnp.where(group == x, pltpu.roll(both, 2 * x, 1), packed)
            return packed

        ez[r] = lax.fori_loop(0, 8, pack, jnp.zeros((64, 128), F32))

    pack_faces(0, u0)
    start(round0[4:])
    first8, last8 = first[:8], last[:8]
    zero8 = jnp.zeros((8, 128), F32)

    def beside_z(u, starts, x0, group_size):
        for j in range(group_size):
            for k, y in enumerate(starts):
                c = [u[x0 + j + 1, h, pl.ds(8 + y, 8), :] for h in range(2)]
                right = [pltpu.roll(c[h], 1, 1) for h in range(2)]
                left = [pltpu.roll(c[h], 127, 1) for h in range(2)]
                zs[j, k, 0] = jnp.where(first8, zero8, right[0]) + jnp.where(last8, left[1], left[0])
                zs[j, k, 1] = jnp.where(first8, right[0], right[1]) + jnp.where(last8, zero8, left[1])

    def relax(u, v, off, starts, x0, group_size):
        def planes(p):
            return [[u[p, h, pl.ds(8 + y, 8), :] for h in range(2)] for y in starts]

        before, here = planes(x0), planes(x0 + 1)
        for j in range(group_size):
            x = x0 + j
            after = planes(x + 2)
            for k, y in enumerate(starts):
                for h in range(2):
                    total = (before[k][h] + after[k][h]) + (here[k][h] + bv[x + 2, h, pl.ds(y, 8), :])
                    total = total + (u[x + 1, h, pl.ds(7 + y, 8), :] + u[x + 1, h, pl.ds(9 + y, 8), :])
                    v[x + off, h, pl.ds(8 + y, 8), :] = (total + zs[j, k, h]) * SEVENTH
            before, here = here, after

    def sweep(u, v, off):
        every = 64 // GI
        count = (8 // NI) * every

        def place(n):
            y = 8 * NI * (n // every)
            return [pl.multiple_of(y + 8 * k, 8) for k in range(NI)], GI * lax.rem(n, every)

        beside_z(u, *place(0), GI)

        def body(n, _):
            relax(u, v, off, *place(n), GI)
            beside_z(u, *place(jnp.minimum(n + 1, count - 1)), GI)
            return 0

        lax.fori_loop(0, count, body, 0)

    def add_halos(r, copies, v, off):
        arrive(copies)
        even = lax.rem(lane, 2) == 0
        zr[r, 0] = jnp.where(even, pltpu.roll(zr[r, 0], 1, 1), pltpu.roll(zr[r, 1], 127, 1)) * SEVENTH
        for side, p in enumerate((off, off + 63)):

            @pl.when(has("gx", 2 * side - 1))
            def _():
                for h in range(2):
                    v[p, h, pl.ds(8, 64), :] = v[p, h, pl.ds(8, 64), :] + hx[r, side, h] * SEVENTH

        def body(n, _):
            for j in range(GH):
                x = GH * n + j
                side = pltpu.roll(zr[r, 0], lax.rem(128 - 2 * x, 128), 1)
                for h in range(2):
                    for k in range(8):
                        at_end = jnp.where(last8 if h else first8, side[8 * k : 8 * k + 8], zero8)
                        if k in (0, 7):
                            at_end = at_end + hy[r, k // 7, x, h] * SEVENTH
                        rows = pl.ds(8 + 8 * k, 8)
                        v[x + off, h, rows, :] = v[x + off, h, rows, :] + at_end
            return 0

        lax.fori_loop(0, 64 // GH, body, 0)

    loads[2].wait()
    loads[3].wait()
    sweep(u0, u1, 1)
    add_halos(0, round0, u1, 1)
    start(round1[:4])
    pack_faces(1, u1)
    start(round1[4:])
    sweep(u1, u2, 3)
    add_halos(1, round1, u2, 3)

    topx = gx == nx - 1

    def restrict(i, _):
        slot = lax.rem(i, 2)
        mid = jnp.where(jnp.logical_and(topx, i == 32), 2.75, 2.5).astype(F32)
        for h in range(2):
            w = [u2[2 * i + k, h, pl.ds(8, 64), :] for k in range(5)]
            b = [bv[2 * i + k, h] for k in range(3)]
            beside = w[1] + w[3]
            at[slot, h, pl.ds(16, 64), :] = 0.25 * beside + 0.5 * w[2]
            load = 0.25 * (b[0] + b[2]) + 0.5 * b[1]
            at[slot, 2 + h, pl.ds(16, 64), :] = (beside - 0.25 * (w[0] + w[4])) + (mid * w[2] - load)
        for h in range(2):
            a1 = [at[slot, h, pl.ds(8 + o, 40, stride=2), :] for o in (-1, 0, 1, 2, 3)]
            a2 = [at[slot, 2 + h, pl.ds(8 + o, 40, stride=2), :] for o in (0, 1, 2)]
            beside = a1[1] + a1[3]
            main = 0.25 * (a2[0] + a2[2]) + 0.5 * a2[1]
            main = main - (0.25 * (a1[0] + a1[4]) + 0.5 * beside) - kc[2] * a1[2]
            qb[i, :, pl.ds(128 * h, 128)] = main
            qb[i, :, pl.ds(256 + 128 * h, 128)] = 0.25 * beside + 0.5 * a1[2]
        return 0


    def restrict_half(n, _):
        i = 17 * n
        lax.fori_loop(0, 18, lambda k, c: restrict(16 * n + k, c), 0, unroll=2)
        got = dot3(qb[pl.ds(i, 17)].reshape(680, 512), wr[...])
        main = got[:, :128].reshape(17, 40, 128)
        gm[pl.ds(i + 3, 17)] = main
        gs[pl.ds(i + 3, 17)] = main
        g2[pl.ds(i + 3, 17), 1] = got[:, 128:].reshape(17, 40, 128)
        return 0

    def half_message(n, dy):
        ya, yn = SEND[dy]
        e = 0 if dy < 0 else 1
        return pltpu.make_async_remote_copy(
            src_ref=gm.at[pl.ds(3 + 17 * n, 17), pl.ds(ya, yn), :],
            dst_ref=rm[XY8.index((0, dy))].at[pl.ds(17 * n, 17)],
            send_sem=h_send.at[n, e], recv_sem=h_recv.at[n, e],
            device_id=target(0, dy, 0), device_id_type=MESH)

    mains = []
    for n, (dx, dy) in enumerate(XY8):
        if dx:
            (xa, xn), (ya, yn) = SEND[dx], SEND[dy]
            mains.append((dx, dy, n, pltpu.make_async_remote_copy(
                src_ref=gm.at[pl.ds(xa, xn), pl.ds(ya, yn), :], dst_ref=rm[n],
                send_sem=m_send.at[n], recv_sem=m_recv.at[n], device_id=target(dx, dy, 0), device_id_type=MESH)))
    mains.sort(key=lambda m: abs(m[1]))

    def half(n, _):
        restrict_half(n, 0)
        for dy in (-1, 1):
            pl.when(has("gy", dy))(lambda: half_message(n, dy).start())
        for dx, dy, _, copy in mains:
            ready = n == (0 if dx < 0 else 1)
            pl.when(jnp.logical_and(ready, has_all(dx, dy, 0)))(copy.start)
        return 0

    lax.fori_loop(0, 2, half, 0)

    edge40 = l40 >= 124
    oct40 = l40 // 8
    for t, (lo, hi) in enumerate(((0, 16), (16, 32), (32, 40))):

        def pack_ends(p, ends):
            main, halo = gm[p], g2[p, 1]
            q = p - 16 * t
            shift = lax.rem(8 * q + 4, 128)
            here = oct40 == q
            return (
                jnp.where(here, pltpu.roll(jnp.where(edge40, halo, main), shift, 1), ends[0]),
                jnp.where(here, pltpu.roll(jnp.where(edge40, main, halo), shift, 1), ends[1]),
            )

        ends = lax.fori_loop(lo, hi, pack_ends, (zero40, zero40), unroll=UE)
        for k in range(2):
            lh[k, t] = ends[k]
            ls[k, t] = ends[k]

    messages = []
    for n, (dx, dy) in enumerate(XY8):
        ya, yn = SEND[dy]
        ta, tn = TSEND[dx]
        messages.append((dx, dy, 0, n, pltpu.make_async_remote_copy(
            src_ref=lh.at[:, pl.ds(ta, tn), pl.ds(ya, yn), :], dst_ref=rl[n],
            send_sem=l_send.at[n], recv_sem=l_recv.at[n], device_id=target(dx, dy, 0), device_id_type=MESH)))
    for n, (dx, dy) in enumerate(XY):
        ya, yn = SEND[dy]
        ta, tn = TSEND[dx]
        for dz in (-1, 1):
            end = 1 if dz > 0 else 0
            messages.append((dx, dy, dz, n, pltpu.make_async_remote_copy(
                src_ref=lh.at[end, pl.ds(ta, tn), pl.ds(ya, yn), :], dst_ref=rz[n].at[1 - end],
                send_sem=z_send.at[n, end], recv_sem=z_recv.at[n, end],
                device_id=target(dx, dy, dz), device_id_type=MESH)))
    messages.sort(key=lambda m: (abs(m[0]) + abs(m[1]) + abs(m[2])))
    for dx, dy, dz, _, copy in messages:
        pl.when(has_all(dx, dy, dz))(copy.start)

    def add_main(dx, dy, n):
        xn, xl = SEND[dx][1], LAND[dx]
        rows = pl.ds(LAND[dy], SEND[dy][1])

        def add(p, _):
            gs[xl + p, rows, :] = gs[xl + p, rows, :] + rm[n][p]
            return 0

        lax.fori_loop(0, xn, add, 0, unroll=min(xn, 17))

    def take_half(dy):
        half_message(0, dy).wait_recv()
        half_message(1, dy).wait_recv()
        add_main(0, dy, XY8.index((0, dy)))

    def take_main(dx, dy, n, copy):
        copy.wait_recv()
        add_main(dx, dy, n)

    def take_ends(dx, dy, dz, n, copy):
        copy.wait_recv()
        rows, tl = pl.ds(LAND[dy], SEND[dy][1]), TLAND[dx]
        for k in (0, 1) if dz == 0 else (0,) if dz > 0 else (1,):
            src = rl[n] if dz == 0 else rz[n]
            for t in range(TSEND[dx][1]):
                ls[k, tl + t, rows, :] = ls[k, tl + t, rows, :] + src[k, t]

    for dy in (-1, 1):
        pl.when(has("gy", -dy))(functools.partial(take_half, dy))
    for dx, dy, n, copy in mains:
        pl.when(has_all(-dx, -dy, 0))(functools.partial(take_main, dx, dy, n, copy))
    for dx, dy, dz, n, copy in messages:
        pl.when(has_all(-dx, -dy, -dz))(functools.partial(take_ends, dx, dy, dz, n, copy))

    begin40 = l40 < 4
    def assemble(p, _):
        t = p // 16
        q = p - 16 * t
        shift = lax.rem(252 - 8 * q, 128)
        low = pltpu.roll(ls[0, t], shift, 1)
        high = pltpu.roll(ls[1, t], shift, 1)
        main = jnp.where(begin40, low, jnp.where(edge40, high, gs[p]))
        halo = jnp.where(begin40, high, jnp.where(edge40, low, zero40))
        g2[p, 0] = main
        g2[p, 1] = halo
        ca[p, 0, pl.ds(8, 40), :] = main * kc[0]
        ca[p, 1, pl.ds(8, 40), :] = halo * kc[1]
        return 0

    lax.fori_loop(0, 40, assemble, 0, unroll=UA)

    zc = jnp.zeros((2, 40, 128), F32)

    def clip(c):
        @pl.when(gx == 0)
        def _():
            for p in range(4):
                c[p, :, pl.ds(8, 40), :] = zc

        @pl.when(gx == nx - 1)
        def _():
            for p in range(36, 40):
                c[p, :, pl.ds(8, 40), :] = zc

    first40 = l40 == 0
    last40 = l40 == 127

    def coarse_sweep(c, v, lo, hi, many):
        def planes(p):
            return [c[p, h, pl.ds(8, 40), :] for h in range(2)]

        def body(n, _):
            p0 = lo + many * n
            before, own = planes(p0 - 1), planes(p0)
            for j in range(many):
                p = p0 + j
                after = planes(p + 1)
                right = [pltpu.roll(own[h], 1, 1) for h in range(2)]
                left = [pltpu.roll(own[h], 127, 1) for h in range(2)]
                for h in range(2):
                    total = (before[h] + after[h]) + (own[h] + g2[p, h])
                    total = total + (c[p, h, pl.ds(7, 40), :] + c[p, h, pl.ds(9, 40), :])
                    total = total + jnp.where(first40, right[1 - h], right[h])
                    total = total + jnp.where(last40, left[1 - h], left[h])
                    v[p, h, pl.ds(8, 40), :] = total * kc[h]
                before, own = own, after
            return 0

        lax.fori_loop(0, (hi - lo) // many, body, 0)
        clip(v)

    clip(ca)
    coarse_sweep(ca, cb, 1, 41, UC[0])
    coarse_sweep(cb, ca, 2, 38, UC[1])
    coarse_sweep(ca, cb, 3, 38, UC[2])

    def prolong_z(n, _):
        i = 11 * n
        block = [cb[pl.ds(3 + i, 11), h, pl.ds(8, 40), :].reshape(440, 128) for h in range(2)]
        got = dot3(jnp.concatenate(block, axis=1), wp[...])
        for h in range(2):
            fz[pl.ds(i, 11), h] = got[:, 128 * h : 128 * h + 128].reshape(11, 40, 128)
        return 0

    lax.fori_loop(0, 3, prolong_z, 0)

    sent(round0)
    sent(round1)
    for n in range(2):
        for dy in (-1, 1):
            pl.when(has("gy", dy))(half_message(n, dy).wait_send)
    for dx, dy, n, copy in mains:
        pl.when(has_all(dx, dy, 0))(copy.wait_send)
    for dx, dy, dz, n, copy in messages:
        pl.when(has_all(dx, dy, dz))(copy.wait_send)


def finish_kernel(u2, fz, out, ot, wt, out_sem):
    def prolong_y(j, slot):
        for h in range(2):
            here = fz[j, h, pl.ds(4, 32), :]
            wt[slot, h, pl.ds(0, 32, stride=2), :] = 0.5 * (fz[j, h, pl.ds(3, 32), :] + here)
            wt[slot, h, pl.ds(1, 32, stride=2), :] = here

    prolong_y(0, 0)

    def outgoing(x, n, h):
        return pltpu.make_async_copy(
            ot.at[pl.ds(x, n), h], out.at[pl.ds(x, n), :, pl.ds(128 * h, 128)], out_sem.at[h])

    def finish(i, _):
        slot = lax.rem(i + 1, 2)
        prolong_y(i + 1, slot)
        for h in range(2):
            here = wt[slot, h]
            mean = 0.5 * (wt[1 - slot, h] + here)
            ot[2 * i, h] = u2[2 * i + 3, h, pl.ds(8, 64), :] + mean
            ot[2 * i + 1, h] = u2[2 * i + 4, h, pl.ds(8, 64), :] + here
        for h in range(2):
            outgoing(2 * i, 2, h).start()
        return 0

    lax.fori_loop(0, 32, finish, 0, unroll=UF)
    for h in range(2):
        outgoing(0, 64, h).wait()


def on_device(start_field, right_side):
    v = pltpu.VMEM
    scratch = [
        v((66, 2, 80, 128), F32), v((66, 2, 80, 128), F32),
        v((69, 2, 64, 128), F32), v((2, 64, 128), F32), v((2, 2, 64, 128), F32),
        v((2, 4, 96, 128), F32), v((34, 40, 512), F32), v((512, 256), BF16), v((256, 256), BF16),
        v((40, 40, 128), F32), v((40, 40, 128), F32), v((2, 3, 40, 128), F32), v((2, 3, 40, 128), F32),
        v((3, 40, 128), F32), v((42, 2, 40, 128), F32), v((42, 2, 56, 128), F32), v((42, 2, 56, 128), F32),
        v((GI, NI, 2, 8, 128), F32),
        v((2, 2, 2, 64, 128), F32), v((2, 2, 64, 2, 8, 128), F32),
    ]
    scratch += [v((SEND[dx][1], SEND[dy][1], 128), F32) for dx, dy in XY8]
    scratch += [v((2, TSEND[dx][1], SEND[dy][1], 128), F32) for dx, dy in XY8]
    scratch += [v((2, TSEND[dx][1], SEND[dy][1], 128), F32) for dx, dy in XY]
    dma = pltpu.SemaphoreType.DMA
    scratch += [dma((4,)), dma((2, 6)), dma((2, 6)), dma((8,)), dma((8,)), dma((8,)), dma((8,)),
                dma((9, 2)), dma((9, 2)), dma((2, 2)), dma((2, 2))]
    anywhere = pl.BlockSpec(memory_space=pltpu.HBM)
    vmem = pl.BlockSpec(memory_space=pltpu.VMEM)
    smoothed, correction = pl.pallas_call(
        kernel,
        out_shape=(v((71, 2, 80, 128), F32), v((33, 2, 40, 128), F32)),
        in_specs=[anywhere, anywhere],
        out_specs=(vmem, vmem),
        scratch_shapes=scratch,
        compiler_params=pltpu.CompilerParams(
            collective_id=0, has_side_effects=True, vmem_limit_bytes=54 * 1024 * 1024),
    )(start_field, right_side)
    return pl.pallas_call(
        finish_kernel,
        out_shape=jax.ShapeDtypeStruct(start_field.shape, F32),
        in_specs=[vmem, vmem],
        out_specs=anywhere,
        scratch_shapes=[v((64, 2, 64, 128), F32), v((2, 2, 64, 128), F32), dma((2,))],
        compiler_params=pltpu.CompilerParams(vmem_limit_bytes=12 * 1024 * 1024),
    )(smoothed, correction)


def solution(mesh):
    placed = P("gx", "gy", "gz")
    return jax.shard_map(on_device, mesh=mesh, in_specs=(placed, placed), out_specs=placed, check_vma=False)
```

```python
import functools

import jax
import jax.numpy as jnp
from jax import lax
from jax.experimental import pallas as pl
from jax.experimental.pallas import tpu as pltpu
from jax.sharding import PartitionSpec as P

MESH = pl.DeviceIdType.MESH
F32 = jnp.float32
BF16 = jnp.bfloat16
SEVENTH = 1.0 / 7.0
UE, UA, UF = 8, 10, 2
NI, GI, GH = 4, 8, 32
UC = (8, 6, 7)
AXES = ("gx", "gy", "gz")
SEND = {-1: (3, 4), 0: (3, 34), 1: (32, 5)}
LAND = {-1: 35, 0: 3, 1: 0}
TSEND = {-1: (0, 1), 0: (0, 3), 1: (2, 1)}
TLAND = {-1: 2, 0: 0, 1: 0}
XY = [(dx, dy) for dx in (-1, 0, 1) for dy in (-1, 0, 1)]
XY8 = [d for d in XY if d != (0, 0)]


def split3(v):
    hi = v.astype(BF16)
    rest = v - hi.astype(F32)
    mid = rest.astype(BF16)
    lo = (rest - mid.astype(F32)).astype(BF16)
    return hi, mid, lo


def dot3(v, weights):
    parts = [jnp.dot(p, weights, preferred_element_type=F32) for p in split3(v)]
    return (parts[2] + parts[1]) + parts[0]


def kernel(s_in, b_in, u2, fz, *scratch):
    (u0, u1, bv, ez, zr, at, qb, wr, wp, gm, gs, lh, ls, kc, g2, ca, cb, zs, hx, hy) = scratch[:20]
    rm = scratch[20:28]
    rl = scratch[28:36]
    rz = scratch[36:45]
    load_sem, f_send, f_recv, m_send, m_recv, l_send, l_recv, z_send, z_recv, h_send, h_recv = scratch[45:]

    gx, gy, gz = (lax.axis_index(a) for a in AXES)
    nx, ny, nz = (lax.axis_size(a) for a in AXES)
    me = {"gx": gx, "gy": gy, "gz": gz}
    size = {"gx": nx, "gy": ny, "gz": nz}

    def has(axis, d):
        if d == 0:
            return True
        return me[axis] < size[axis] - 1 if d > 0 else me[axis] > 0

    def has_all(dx, dy, dz):
        ok = None
        for axis, d in zip(AXES, (dx, dy, dz)):
            if d:
                here = has(axis, d)
                ok = here if ok is None else jnp.logical_and(ok, here)
        return ok

    def target(dx, dy, dz):
        return {a: me[a] + d for a, d in zip(AXES, (dx, dy, dz))}

    loads = []
    for h in range(2):
        lanes = pl.ds(128 * h, 128)
        loads.append(pltpu.make_async_copy(s_in.at[:, :, lanes], u0.at[pl.ds(1, 64), h, pl.ds(8, 64), :], load_sem.at[h]))
    for h in range(2):
        lanes = pl.ds(128 * h, 128)
        loads.append(pltpu.make_async_copy(b_in.at[:, :, lanes], bv.at[pl.ds(2, 64), h], load_sem.at[2 + h]))
    loads[0].start()
    loads[1].start()

    barrier = pltpu.get_barrier_semaphore()
    count = jnp.int32(0)
    for axis in AXES:
        for d in (-1, 1):
            ok = has(axis, d)
            count = count + ok.astype(jnp.int32)

            @pl.when(ok)
            def _():
                pl.semaphore_signal(barrier, inc=1, device_id={axis: me[axis] + d}, device_id_type=MESH)

    lane = lax.broadcasted_iota(jnp.int32, (64, 128), 1)
    first = lane == 0
    last = lane == 127
    group = lax.rem((lane + 1) // 2, 64)

    zplane = jnp.zeros((2, 80, 128), F32)
    zrow = jnp.zeros((1, 128), F32)
    for u in (u0, u1):
        u[0] = zplane
        u[65] = zplane

    def zero_rows(x, _):
        for h in range(2):
            for u in (u0, u1):
                u[x + 1, h, pl.ds(7, 1), :] = zrow
                u[x + 1, h, pl.ds(72, 1), :] = zrow
            for r in range(2):
                hy[r, 0, x, h, pl.ds(1, 7), :] = jnp.zeros((7, 128), F32)
                hy[r, 1, x, h, pl.ds(0, 7), :] = jnp.zeros((7, 128), F32)
        return 0

    lax.fori_loop(0, 64, zero_rows, 0, unroll=2)

    def zero_halo(side):
        def body(x, _):
            for r in range(2):
                for h in range(2):
                    hy[r, side, x, h, pl.ds(7 * side, 1), :] = zrow
            return 0

        lax.fori_loop(0, 64, body, 0)

    for side in range(2):
        d = 2 * side - 1

        @pl.when(jnp.logical_not(has("gy", d)))
        def _():
            zero_halo(side)

        @pl.when(jnp.logical_not(has("gz", d)))
        def _():
            for r in range(2):
                zr[r, side] = jnp.zeros((64, 128), F32)

    for p in (0, 1, 2, 67, 68, 69, 70):
        u2[p] = zplane
    for p in (0, 1, 66, 67, 68):
        bv[p] = jnp.zeros((2, 64, 128), F32)
    at[...] = jnp.zeros(at.shape, F32)

    def coarse_of(column):
        inner = column - 128
        return jnp.where(column < 128, column, jnp.where(inner >= 64, inner - 128, inner + 128))

    zi = lax.broadcasted_iota(jnp.int32, (256, 256), 0)
    kci = coarse_of(lax.broadcasted_iota(jnp.int32, (256, 256), 1))
    d = zi - 2 * kci
    zero = jnp.zeros((256, 256), F32)
    plain = jnp.where(d == 1, -2.0, jnp.where((d == 0) | (d == 2), -1.0, zero))
    topz = (gz == nz - 1).astype(F32)
    edge = jnp.where((zi == 255) & (kci == 127), topz, zero)
    around = jnp.where((d >= 0) & (d <= 2), 2.0, jnp.where((d == -1) | (d == 3), 1.0, zero)) - edge
    wr[pl.ds(0, 256), :] = plain.astype(BF16)
    wr[pl.ds(256, 256), :] = around.astype(BF16)
    kr = coarse_of(lax.broadcasted_iota(jnp.int32, (256, 256), 0))
    d = lax.broadcasted_iota(jnp.int32, (256, 256), 1) - 2 * kr
    wp[...] = jnp.where(d == 1, 1.0, jnp.where((d == 0) | (d == 2), 0.5, zero)).astype(BF16)

    r40 = lax.broadcasted_iota(jnp.int32, (40, 128), 0)
    l40 = lax.broadcasted_iota(jnp.int32, (40, 128), 1)
    zero40 = jnp.zeros((40, 128), F32)
    low_y = jnp.where(gy > 0, 0, 4)
    high_y = jnp.where(gy < ny - 1, 40, 36)
    low_z = jnp.where(gz > 0, 124, 128)
    high_z = jnp.where(gz < nz - 1, 4, 0)
    rows_in = jnp.where((r40 >= low_y) & (r40 < high_y), SEVENTH, zero40)
    kc[0] = rows_in
    for p in (0, 1, 2, 37, 38, 39):
        gm[p] = zero40
        gs[p] = zero40
        g2[p, 1] = zero40
    kc[1] = jnp.where((l40 >= low_z) | (l40 < high_z), rows_in, zero40)
    topy = (gy == ny - 1).astype(F32)
    kc[2] = 0.5 - jnp.where(r40 == 35, 0.25 * topy, zero40)

    zpad = jnp.zeros((42, 2, 8, 128), F32)
    for c in (ca, cb):
        c[:, :, pl.ds(0, 8), :] = zpad
        c[:, :, pl.ds(48, 8), :] = zpad

    def faces(r, u):
        x_in = (slice(None), pl.ds(8, 64), slice(None))
        xs = pl.ds(1, 64)
        every = slice(None)
        plan = [
            ("gx", 1, u.at[(64,) + x_in], hx.at[r, 0]),
            ("gx", -1, u.at[(1,) + x_in], hx.at[r, 1]),
            ("gy", 1, u.at[xs, every, pl.ds(71, 1), every], hy.at[r, 0, every, every, pl.ds(0, 1), every]),
            ("gy", -1, u.at[xs, every, pl.ds(8, 1), every], hy.at[r, 1, every, every, pl.ds(7, 1), every]),
            ("gz", 1, ez.at[r], zr.at[r, 0]),
            ("gz", -1, ez.at[r], zr.at[r, 1]),
        ]
        done = []
        for k, (axis, dd, src, dst) in enumerate(plan):
            copy = pltpu.make_async_remote_copy(
                src_ref=src, dst_ref=dst, send_sem=f_send.at[r, k], recv_sem=f_recv.at[r, k],
                device_id={axis: me[axis] + dd}, device_id_type=MESH,
            )
            done.append((axis, dd, copy))
        return done

    def start(copies):
        for axis, dd, copy in copies:
            pl.when(has(axis, dd))(copy.start)

    def arrive(copies):
        for axis, dd, copy in copies:
            pl.when(has(axis, -dd))(copy.wait_recv)

    def sent(copies):
        for axis, dd, copy in copies:
            pl.when(has(axis, dd))(copy.wait_send)

    round0, round1 = faces(0, u0), faces(1, u1)

    loads[0].wait()
    loads[1].wait()
    loads[2].start()
    loads[3].start()
    pl.semaphore_wait(barrier, count)
    start(round0[:4])

    first8, last8 = first[:8], last[:8]

    def pack_faces(r, u):
        def pack(n, packed):
            for j in range(32):
                x = 32 * n + j
                both = jnp.where(first, u[x + 1, 0, pl.ds(8, 64), :], u[x + 1, 1, pl.ds(8, 64), :])
                packed = jnp.where(group == x, pltpu.roll(both, 2 * x, 1), packed)
            return packed

        ez[r] = lax.fori_loop(0, 2, pack, jnp.zeros((64, 128), F32))

    pack_faces(0, u0)
    start(round0[4:])
    first8, last8 = first[:8], last[:8]
    zero8 = jnp.zeros((8, 128), F32)

    def beside_z(u, starts, x0, group_size):
        for j in range(group_size):
            for k, y in enumerate(starts):
                c = [u[x0 + j + 1, h, pl.ds(8 + y, 8), :] for h in range(2)]
                right = [pltpu.roll(c[h], 1, 1) for h in range(2)]
                left = [pltpu.roll(c[h], 127, 1) for h in range(2)]
                zs[j, k, 0] = jnp.where(first8, zero8, right[0]) + jnp.where(last8, left[1], left[0])
                zs[j, k, 1] = jnp.where(first8, right[0], right[1]) + jnp.where(last8, zero8, left[1])

    def relax(u, v, off, starts, x0, group_size):
        def planes(p):
            return [[u[p, h, pl.ds(8 + y, 8), :] for h in range(2)] for y in starts]

        before, here = planes(x0), planes(x0 + 1)
        for j in range(group_size):
            x = x0 + j
            after = planes(x + 2)
            for k, y in enumerate(starts):
                for h in range(2):
                    total = (before[k][h] + after[k][h]) + (here[k][h] + bv[x + 2, h, pl.ds(y, 8), :])
                    total = total + (u[x + 1, h, pl.ds(7 + y, 8), :] + u[x + 1, h, pl.ds(9 + y, 8), :])
                    v[x + off, h, pl.ds(8 + y, 8), :] = (total + zs[j, k, h]) * SEVENTH
            before, here = here, after

    def sweep(u, v, off):
        every = 64 // GI
        count = (8 // NI) * every

        def place(n):
            y = 8 * NI * (n // every)
            return [pl.multiple_of(y + 8 * k, 8) for k in range(NI)], GI * lax.rem(n, every)

        beside_z(u, *place(0), GI)

        def body(n, _):
            relax(u, v, off, *place(n), GI)
            beside_z(u, *place(jnp.minimum(n + 1, count - 1)), GI)
            return 0

        lax.fori_loop(0, count, body, 0)

    def add_halos(r, copies, v, off):
        arrive(copies)
        even = lax.rem(lane, 2) == 0
        zr[r, 0] = jnp.where(even, pltpu.roll(zr[r, 0], 1, 1), pltpu.roll(zr[r, 1], 127, 1)) * SEVENTH
        for side, p in enumerate((off, off + 63)):

            @pl.when(has("gx", 2 * side - 1))
            def _():
                for h in range(2):
                    v[p, h, pl.ds(8, 64), :] = v[p, h, pl.ds(8, 64), :] + hx[r, side, h] * SEVENTH

        def body(n, _):
            for j in range(GH):
                x = GH * n + j
                side = pltpu.roll(zr[r, 0], lax.rem(128 - 2 * x, 128), 1)
                for h in range(2):
                    for k in range(8):
                        at_end = jnp.where(last8 if h else first8, side[8 * k : 8 * k + 8], zero8)
                        if k in (0, 7):
                            at_end = at_end + hy[r, k // 7, x, h] * SEVENTH
                        rows = pl.ds(8 + 8 * k, 8)
                        v[x + off, h, rows, :] = v[x + off, h, rows, :] + at_end
            return 0

        lax.fori_loop(0, 64 // GH, body, 0)

    loads[2].wait()
    loads[3].wait()
    sweep(u0, u1, 1)
    add_halos(0, round0, u1, 1)
    start(round1[:4])
    pack_faces(1, u1)
    start(round1[4:])
    sweep(u1, u2, 3)
    add_halos(1, round1, u2, 3)

    topx = gx == nx - 1

    def restrict(i, _):
        slot = lax.rem(i, 2)
        mid = jnp.where(jnp.logical_and(topx, i == 32), 2.75, 2.5).astype(F32)
        for h in range(2):
            w = [u2[2 * i + k, h, pl.ds(8, 64), :] for k in range(5)]
            b = [bv[2 * i + k, h] for k in range(3)]
            beside = w[1] + w[3]
            at[slot, h, pl.ds(16, 64), :] = 0.25 * beside + 0.5 * w[2]
            load = 0.25 * (b[0] + b[2]) + 0.5 * b[1]
            at[slot, 2 + h, pl.ds(16, 64), :] = (beside - 0.25 * (w[0] + w[4])) + (mid * w[2] - load)
        for h in range(2):
            a1 = [at[slot, h, pl.ds(8 + o, 40, stride=2), :] for o in (-1, 0, 1, 2, 3)]
            a2 = [at[slot, 2 + h, pl.ds(8 + o, 40, stride=2), :] for o in (0, 1, 2)]
            beside = a1[1] + a1[3]
            main = 0.25 * (a2[0] + a2[2]) + 0.5 * a2[1]
            main = main - (0.25 * (a1[0] + a1[4]) + 0.5 * beside) - kc[2] * a1[2]
            qb[i, :, pl.ds(128 * h, 128)] = main
            qb[i, :, pl.ds(256 + 128 * h, 128)] = 0.25 * beside + 0.5 * a1[2]
        return 0


    def restrict_half(n, _):
        i = 17 * n
        lax.fori_loop(0, 18, lambda k, c: restrict(16 * n + k, c), 0, unroll=2)
        got = dot3(qb[pl.ds(i, 17)].reshape(680, 512), wr[...])
        main = got[:, :128].reshape(17, 40, 128)
        gm[pl.ds(i + 3, 17)] = main
        gs[pl.ds(i + 3, 17)] = main
        g2[pl.ds(i + 3, 17), 1] = got[:, 128:].reshape(17, 40, 128)
        return 0

    def half_message(n, dy):
        ya, yn = SEND[dy]
        e = 0 if dy < 0 else 1
        return pltpu.make_async_remote_copy(
            src_ref=gm.at[pl.ds(3 + 17 * n, 17), pl.ds(ya, yn), :],
            dst_ref=rm[XY8.index((0, dy))].at[pl.ds(17 * n, 17)],
            send_sem=h_send.at[n, e], recv_sem=h_recv.at[n, e],
            device_id=target(0, dy, 0), device_id_type=MESH)

    mains = []
    for n, (dx, dy) in enumerate(XY8):
        if dx:
            (xa, xn), (ya, yn) = SEND[dx], SEND[dy]
            mains.append((dx, dy, n, pltpu.make_async_remote_copy(
                src_ref=gm.at[pl.ds(xa, xn), pl.ds(ya, yn), :], dst_ref=rm[n],
                send_sem=m_send.at[n], recv_sem=m_recv.at[n], device_id=target(dx, dy, 0), device_id_type=MESH)))
    mains.sort(key=lambda m: abs(m[1]))

    def half(n, _):
        restrict_half(n, 0)
        for dy in (-1, 1):
            pl.when(has("gy", dy))(lambda: half_message(n, dy).start())
        for dx, dy, _, copy in mains:
            ready = n == (0 if dx < 0 else 1)
            pl.when(jnp.logical_and(ready, has_all(dx, dy, 0)))(copy.start)
        return 0

    lax.fori_loop(0, 2, half, 0)

    edge40 = l40 >= 124
    oct40 = l40 // 8
    for t, (lo, hi) in enumerate(((0, 16), (16, 32), (32, 40))):

        def pack_ends(p, ends):
            main, halo = gm[p], g2[p, 1]
            q = p - 16 * t
            shift = lax.rem(8 * q + 4, 128)
            here = oct40 == q
            return (
                jnp.where(here, pltpu.roll(jnp.where(edge40, halo, main), shift, 1), ends[0]),
                jnp.where(here, pltpu.roll(jnp.where(edge40, main, halo), shift, 1), ends[1]),
            )

        ends = lax.fori_loop(lo, hi, pack_ends, (zero40, zero40), unroll=UE)
        for k in range(2):
            lh[k, t] = ends[k]
            ls[k, t] = ends[k]

    messages = []
    for n, (dx, dy) in enumerate(XY8):
        ya, yn = SEND[dy]
        ta, tn = TSEND[dx]
        messages.append((dx, dy, 0, n, pltpu.make_async_remote_copy(
            src_ref=lh.at[:, pl.ds(ta, tn), pl.ds(ya, yn), :], dst_ref=rl[n],
            send_sem=l_send.at[n], recv_sem=l_recv.at[n], device_id=target(dx, dy, 0), device_id_type=MESH)))
    for n, (dx, dy) in enumerate(XY):
        ya, yn = SEND[dy]
        ta, tn = TSEND[dx]
        for dz in (-1, 1):
            end = 1 if dz > 0 else 0
            messages.append((dx, dy, dz, n, pltpu.make_async_remote_copy(
                src_ref=lh.at[end, pl.ds(ta, tn), pl.ds(ya, yn), :], dst_ref=rz[n].at[1 - end],
                send_sem=z_send.at[n, end], recv_sem=z_recv.at[n, end],
                device_id=target(dx, dy, dz), device_id_type=MESH)))
    messages.sort(key=lambda m: (abs(m[0]) + abs(m[1]) + abs(m[2])))
    for dx, dy, dz, _, copy in messages:
        pl.when(has_all(dx, dy, dz))(copy.start)

    def add_main(dx, dy, n):
        xn, xl = SEND[dx][1], LAND[dx]
        rows = pl.ds(LAND[dy], SEND[dy][1])

        def add(p, _):
            gs[xl + p, rows, :] = gs[xl + p, rows, :] + rm[n][p]
            return 0

        lax.fori_loop(0, xn, add, 0, unroll=min(xn, 17))

    def take_half(dy):
        half_message(0, dy).wait_recv()
        half_message(1, dy).wait_recv()
        add_main(0, dy, XY8.index((0, dy)))

    def take_main(dx, dy, n, copy):
        copy.wait_recv()
        add_main(dx, dy, n)

    def take_ends(dx, dy, dz, n, copy):
        copy.wait_recv()
        rows, tl = pl.ds(LAND[dy], SEND[dy][1]), TLAND[dx]
        for k in (0, 1) if dz == 0 else (0,) if dz > 0 else (1,):
            src = rl[n] if dz == 0 else rz[n]
            for t in range(TSEND[dx][1]):
                ls[k, tl + t, rows, :] = ls[k, tl + t, rows, :] + src[k, t]

    for dy in (-1, 1):
        pl.when(has("gy", -dy))(functools.partial(take_half, dy))
    for dx, dy, n, copy in mains:
        pl.when(has_all(-dx, -dy, 0))(functools.partial(take_main, dx, dy, n, copy))
    for dx, dy, dz, n, copy in messages:
        pl.when(has_all(-dx, -dy, -dz))(functools.partial(take_ends, dx, dy, dz, n, copy))

    begin40 = l40 < 4
    def assemble(p, _):
        t = p // 16
        q = p - 16 * t
        shift = lax.rem(252 - 8 * q, 128)
        low = pltpu.roll(ls[0, t], shift, 1)
        high = pltpu.roll(ls[1, t], shift, 1)
        main = jnp.where(begin40, low, jnp.where(edge40, high, gs[p]))
        halo = jnp.where(begin40, high, jnp.where(edge40, low, zero40))
        g2[p, 0] = main
        g2[p, 1] = halo
        ca[p, 0, pl.ds(8, 40), :] = main * kc[0]
        ca[p, 1, pl.ds(8, 40), :] = halo * kc[1]
        return 0

    lax.fori_loop(0, 40, assemble, 0, unroll=UA)

    zc = jnp.zeros((2, 40, 128), F32)

    def clip(c):
        @pl.when(gx == 0)
        def _():
            for p in range(4):
                c[p, :, pl.ds(8, 40), :] = zc

        @pl.when(gx == nx - 1)
        def _():
            for p in range(36, 40):
                c[p, :, pl.ds(8, 40), :] = zc

    first40 = l40 == 0
    last40 = l40 == 127

    def coarse_sweep(c, v, lo, hi, many):
        def planes(p):
            return [c[p, h, pl.ds(8, 40), :] for h in range(2)]

        def body(n, _):
            p0 = lo + many * n
            before, own = planes(p0 - 1), planes(p0)
            for j in range(many):
                p = p0 + j
                after = planes(p + 1)
                right = [pltpu.roll(own[h], 1, 1) for h in range(2)]
                left = [pltpu.roll(own[h], 127, 1) for h in range(2)]
                for h in range(2):
                    total = (before[h] + after[h]) + (own[h] + g2[p, h])
                    total = total + (c[p, h, pl.ds(7, 40), :] + c[p, h, pl.ds(9, 40), :])
                    total = total + jnp.where(first40, right[1 - h], right[h])
                    total = total + jnp.where(last40, left[1 - h], left[h])
                    v[p, h, pl.ds(8, 40), :] = total * kc[h]
                before, own = own, after
            return 0

        lax.fori_loop(0, (hi - lo) // many, body, 0)
        clip(v)

    clip(ca)
    coarse_sweep(ca, cb, 1, 41, UC[0])
    coarse_sweep(cb, ca, 2, 38, UC[1])
    coarse_sweep(ca, cb, 3, 38, UC[2])

    def prolong_z(n, _):
        i = 11 * n
        block = [cb[pl.ds(3 + i, 11), h, pl.ds(8, 40), :].reshape(440, 128) for h in range(2)]
        got = dot3(jnp.concatenate(block, axis=1), wp[...])
        for h in range(2):
            fz[pl.ds(i, 11), h] = got[:, 128 * h : 128 * h + 128].reshape(11, 40, 128)
        return 0

    lax.fori_loop(0, 3, prolong_z, 0)

    sent(round0)
    sent(round1)
    for n in range(2):
        for dy in (-1, 1):
            pl.when(has("gy", dy))(half_message(n, dy).wait_send)
    for dx, dy, n, copy in mains:
        pl.when(has_all(dx, dy, 0))(copy.wait_send)
    for dx, dy, dz, n, copy in messages:
        pl.when(has_all(dx, dy, dz))(copy.wait_send)


def finish_kernel(u2, fz, out, ot, wt, out_sem):
    def prolong_y(j, slot):
        for h in range(2):
            here = fz[j, h, pl.ds(4, 32), :]
            wt[slot, h, pl.ds(0, 32, stride=2), :] = 0.5 * (fz[j, h, pl.ds(3, 32), :] + here)
            wt[slot, h, pl.ds(1, 32, stride=2), :] = here

    prolong_y(0, 0)

    def outgoing(x, n, h):
        return pltpu.make_async_copy(
            ot.at[pl.ds(x, n), h], out.at[pl.ds(x, n), :, pl.ds(128 * h, 128)], out_sem.at[h])

    def finish(i, _):
        slot = lax.rem(i + 1, 2)
        prolong_y(i + 1, slot)
        for h in range(2):
            here = wt[slot, h]
            mean = 0.5 * (wt[1 - slot, h] + here)
            ot[2 * i, h] = u2[2 * i + 3, h, pl.ds(8, 64), :] + mean
            ot[2 * i + 1, h] = u2[2 * i + 4, h, pl.ds(8, 64), :] + here
        for h in range(2):
            outgoing(2 * i, 2, h).start()
        return 0

    lax.fori_loop(0, 32, finish, 0, unroll=UF)
    for h in range(2):
        outgoing(0, 64, h).wait()


def on_device(start_field, right_side):
    v = pltpu.VMEM
    scratch = [
        v((66, 2, 80, 128), F32), v((66, 2, 80, 128), F32),
        v((69, 2, 64, 128), F32), v((2, 64, 128), F32), v((2, 2, 64, 128), F32),
        v((2, 4, 96, 128), F32), v((34, 40, 512), F32), v((512, 256), BF16), v((256, 256), BF16),
        v((40, 40, 128), F32), v((40, 40, 128), F32), v((2, 3, 40, 128), F32), v((2, 3, 40, 128), F32),
        v((3, 40, 128), F32), v((42, 2, 40, 128), F32), v((42, 2, 56, 128), F32), v((42, 2, 56, 128), F32),
        v((GI, NI, 2, 8, 128), F32),
        v((2, 2, 2, 64, 128), F32), v((2, 2, 64, 2, 8, 128), F32),
    ]
    scratch += [v((SEND[dx][1], SEND[dy][1], 128), F32) for dx, dy in XY8]
    scratch += [v((2, TSEND[dx][1], SEND[dy][1], 128), F32) for dx, dy in XY8]
    scratch += [v((2, TSEND[dx][1], SEND[dy][1], 128), F32) for dx, dy in XY]
    dma = pltpu.SemaphoreType.DMA
    scratch += [dma((4,)), dma((2, 6)), dma((2, 6)), dma((8,)), dma((8,)), dma((8,)), dma((8,)),
                dma((9, 2)), dma((9, 2)), dma((2, 2)), dma((2, 2))]
    anywhere = pl.BlockSpec(memory_space=pltpu.HBM)
    vmem = pl.BlockSpec(memory_space=pltpu.VMEM)
    smoothed, correction = pl.pallas_call(
        kernel,
        out_shape=(v((71, 2, 80, 128), F32), v((33, 2, 40, 128), F32)),
        in_specs=[anywhere, anywhere],
        out_specs=(vmem, vmem),
        scratch_shapes=scratch,
        compiler_params=pltpu.CompilerParams(
            collective_id=0, has_side_effects=True, vmem_limit_bytes=54 * 1024 * 1024),
    )(start_field, right_side)
    return pl.pallas_call(
        finish_kernel,
        out_shape=jax.ShapeDtypeStruct(start_field.shape, F32),
        in_specs=[vmem, vmem],
        out_specs=anywhere,
        scratch_shapes=[v((64, 2, 64, 128), F32), v((2, 2, 64, 128), F32), dma((2,))],
        compiler_params=pltpu.CompilerParams(vmem_limit_bytes=12 * 1024 * 1024),
    )(smoothed, correction)


def solution(mesh):
    placed = P("gx", "gy", "gz")
    return jax.shard_map(on_device, mesh=mesh, in_specs=(placed, placed), out_specs=placed, check_vma=False)
```
